32 devices in a mesh: dp: 8 (over z, x), tensor: 4 (over y, core).
Axes of the slice: x: 2, y: 2, z: 4, core: 2. Of those that a mesh axis runs over, the one named last changes fastest.
Arguments:
- patches: bfloat16 [64, 196, 768], P(('dp', 'tensor')), may hold values from -6 to 6
- labels: int32 [64], P(('dp', 'tensor')), may hold values from 0 to 999
- image_count: int32 [8], replicated, may hold values from 1 to 8, as said below
- attn_weight: float32 [3, 768, 4, 768], P(None, 'dp', None, 'tensor'), may hold values from -0.21875 to 0.21875
- attn_rows: float32 [3, 4, 768], P(None, None, 'dp'), may hold values from 7.947286e-08 to 7.947286e-05
- attn_cols: float32 [3, 4, 768], P(None, None, 'tensor'), may hold values from 7.947286e-08 to 7.947286e-05
- mlp_weight: float32 [3, 2, 768, 3072], P(None, None, 'dp', 'tensor'), may hold values from -0.21875 to 0.21875
- mlp_rows: float32 [3, 2, 768], P(None, None, 'dp'), may hold values from 7.947286e-08 to 7.947286e-05
- mlp_cols: float32 [3, 2, 3072], P(None, None, 'tensor'), may hold values from 7.947286e-08 to 7.947286e-05
- patch_weight: float32 [768, 768], P(('dp', 'tensor')), may hold values from -0.21875 to 0.21875
- patch_rows: float32 [768], P(('dp', 'tensor')), may hold values from 2.6490954e-09 to 2.6490952e-06
- patch_cols: float32 [768], replicated, may hold values from 2.6490954e-09 to 2.6490952e-06
- embed_table: float32 [768, 198], P(('dp', 'tensor')), may hold values from -3 to 3
- embed_rows: float32 [768], P(('dp', 'tensor')), may hold values from 2.6490954e-09 to 2.6490952e-06
- embed_cols: float32 [198], replicated, may hold values from 2.6490954e-09 to 2.6490952e-06
- head_weight: float32 [768, 1000], P(('dp', 'tensor')), may hold values from -0.4375 to 0.4375
- head_rows: float32 [768], P(('dp', 'tensor')), may hold values from 1.5625e-06 to 0.0015625
- head_cols: float32 [1000], replicated, may hold values from 1.5625e-06 to 0.0015625
- split_vec: float32 [3, 2, 768], P(None, None, 'tensor'), may hold values from -2 to 2
- split_sq: float32 [3, 2, 768], P(None, None, 'tensor'), may hold values from 6.1035156e-05 to 0.00024414062
- hidden_bias: float32 [3, 3072], P(None, 'tensor'), may hold values from -2 to 2
- hidden_sq: float32 [3, 3072], P(None, 'tensor'), may hold values from 6.1035156e-05 to 0.00024414062
- shared_vec: float32 [20, 768], replicated, may hold values from 0.25 to 1.75
- shared_sq: float32 [20, 768], replicated, may hold values from 6.1035156e-05 to 0.00024414062
- head_bias: float32 [1000], replicated, may hold values from -3 to 3
- head_bias_sq: float32 [1000], replicated, may hold values from 1e-06 to 4e-06
Outputs:
- mean_loss: float32 [], replicated
- attn_new: float32 [3, 768, 4, 768], P(None, 'dp', None, 'tensor')
- attn_rows_new: float32 [3, 4, 768], P(None, None, 'dp')
- attn_cols_new: float32 [3, 4, 768], P(None, None, 'tensor')
- mlp_new: float32 [3, 2, 768, 3072], P(None, None, 'dp', 'tensor')
- mlp_rows_new: float32 [3, 2, 768], P(None, None, 'dp')
- mlp_cols_new: float32 [3, 2, 3072], P(None, None, 'tensor')
- patch_new: float32 [768, 768], P(('dp', 'tensor'))
- patch_rows_new: float32 [768], P(('dp', 'tensor'))
- patch_cols_new: float32 [768], replicated
- embed_new: float32 [768, 198], P(('dp', 'tensor'))
- embed_rows_new: float32 [768], P(('dp', 'tensor'))
- embed_cols_new: float32 [198], replicated
- head_new: float32 [768, 1000], P(('dp', 'tensor'))
- head_rows_new: float32 [768], P(('dp', 'tensor'))
- head_cols_new: float32 [1000], replicated
- split_new: float32 [3, 2, 768], P(None, None, 'tensor')
- split_sq_new: float32 [3, 2, 768], P(None, None, 'tensor')
- hidden_new: float32 [3, 3072], P(None, 'tensor')
- hidden_sq_new: float32 [3, 3072], P(None, 'tensor')
- shared_new: float32 [20, 768], replicated
- shared_sq_new: float32 [20, 768], replicated
- head_bias_new: float32 [1000], replicated
- head_bias_sq_new: float32 [1000], replicated
The draws below stay inside these ranges and needn't reach their ends.
Inputs may be any that keep to these rules, and one draw needn't show every extreme that they name: Image slot s of dp index i holds a given image when s < image_count[i]; some index holds 8 images and some holds one.
All inputs are finite; a program needn't handle non-finite values.
Results may differ from the reference program's by a relative error of at most 0.014.
Values may be sent and summed in bfloat16 or wider, within the bound.
A program may use at most 256 MiB of HBM per device.

```python
import math
import jax
import jax.numpy as jnp
from jax import lax

D = 768
HEADS = 12
HEAD_DIM = 64
FF = 3072
PATCH = 768
CLASSES = 1000
TOK_IMG = 197
LAYERS = 3
SEQ = 200
SLOTS = 8
NPATCH = 196
EXTRA = 198
IMAGES = 64
N_DP = 8


def draw_image_count(key, part):
    first_key, second_key = jax.random.split(jax.random.fold_in(key, 11))
    counts = jax.random.randint(first_key, (N_DP,), 1, SLOTS + 1)
    ranking = jax.random.permutation(second_key, N_DP)
    counts = counts.at[ranking[0]].set(SLOTS)
    counts = counts.at[ranking[1]].set(1)
    return counts.astype(jnp.int32)


def place_ends(entries, key, smallest, high):
    index_at = [jax.random.randint(jax.random.fold_in(key, axis), (), 0, length) for axis, length in enumerate(entries.shape)]
    main_axis = entries.shape.index(max(entries.shape))
    next_to = index_at[:main_axis] + [(index_at[main_axis] + 1) % entries.shape[main_axis]] + index_at[main_axis + 1:]
    return entries.at[tuple(index_at)].set(smallest).at[tuple(next_to)].set(high)


def block_scale(rng, dims, cuts, least, high):
    gain, own = 1.0, jax.random.fold_in(rng, 6)
    for dim, shards_of in cuts:
        steps = jnp.exp(jax.random.uniform(jax.random.fold_in(own, dim), (shards_of,), jnp.float32, least / len(cuts), high / len(cuts)))
        gain = gain * jnp.repeat(steps, dims[dim] // shards_of).reshape([-1 if axis == dim else 1 for axis in range(len(dims))])
    return gain


def normal_values(rng, dims, scale, most, cuts=(), dtype=jnp.bfloat16):
    gain = block_scale(rng, dims, cuts, -0.22, 0.18) if cuts else 1.0
    entries = jax.random.normal(rng, dims, jnp.float32) * scale * gain
    return jnp.minimum(jnp.maximum(entries, -most), most).astype(dtype)


def setup_inputs(seed: int = 0) -> dict:
    arg_keys = jax.random.split(jax.random.key(seed), 27)
    return {
        "patches": normal_values(arg_keys[0], (IMAGES, NPATCH, PATCH), 1.0, 6.0, ((0, 32),)),
        "labels": place_ends(jax.random.randint(arg_keys[1], (IMAGES,), 0, CLASSES), jax.random.fold_in(arg_keys[1], 1), 0, CLASSES - 1).astype(jnp.int32),
        "image_count": draw_image_count(jax.random.fold_in(arg_keys[26], 71), 0),
        "attn_weight": normal_values(arg_keys[3], (LAYERS, D, 4, D), D ** -0.5, 0.21875, ((1, 8), (3, 4)), jnp.float32),
        "attn_rows": jnp.clip(jnp.exp(math.log(7.947286212584004e-05) - 6.9077553 * jax.random.uniform(arg_keys[4], (LAYERS, 4, D), jnp.float32) ** block_scale(arg_keys[4], (LAYERS, 4, D), ((2, 8),), -0.2, 0.2)), 7.947286206899662e-08, 7.947286212584004e-05),
        "attn_cols": jnp.clip(jnp.exp(math.log(7.947286212584004e-05) - 6.9077553 * jax.random.uniform(arg_keys[5], (LAYERS, 4, D), jnp.float32) ** block_scale(arg_keys[5], (LAYERS, 4, D), ((2, 4),), -0.2, 0.2)), 7.947286206899662e-08, 7.947286212584004e-05),
        "mlp_weight": normal_values(arg_keys[6], (LAYERS, 2, D, FF), D ** -0.5, 0.21875, ((2, 8), (3, 4)), jnp.float32),
        "mlp_rows": jnp.clip(jnp.exp(math.log(7.947286212584004e-05) - 6.9077553 * jax.random.uniform(arg_keys[7], (LAYERS, 2, D), jnp.float32) ** block_scale(arg_keys[7], (LAYERS, 2, D), ((2, 8),), -0.2, 0.2)), 7.947286206899662e-08, 7.947286212584004e-05),
        "mlp_cols": jnp.clip(jnp.exp(math.log(7.947286212584004e-05) - 6.9077553 * jax.random.uniform(arg_keys[8], (LAYERS, 2, FF), jnp.float32) ** block_scale(arg_keys[8], (LAYERS, 2, FF), ((2, 4),), -0.2, 0.2)), 7.947286206899662e-08, 7.947286212584004e-05),
        "patch_weight": normal_values(arg_keys[9], (PATCH, D), PATCH ** -0.5, 0.21875, ((0, 32),), jnp.float32),
        "patch_rows": jnp.clip(jnp.exp(math.log(2.6490952222957276e-06) - 6.9077552 * jax.random.uniform(arg_keys[10], (PATCH,), jnp.float32) ** block_scale(arg_keys[10], (PATCH,), ((0, 32),), -0.2, 0.2)), 2.6490953874969136e-09, 2.6490952222957276e-06),
        "patch_cols": jnp.clip(jnp.exp(jax.random.uniform(arg_keys[11], (D,), jnp.float32, math.log(2.6490953874969136e-09), math.log(2.6490952222957276e-06))), 2.6490953874969136e-09, 2.6490952222957276e-06),
        "embed_table": normal_values(arg_keys[12], (D, EXTRA), 0.5, 3.0, ((0, 32),), jnp.float32),
        "embed_rows": jnp.clip(jnp.exp(math.log(2.6490952222957276e-06) - 6.9077552 * jax.random.uniform(arg_keys[13], (D,), jnp.float32) ** block_scale(arg_keys[13], (D,), ((0, 32),), -0.2, 0.2)), 2.6490953874969136e-09, 2.6490952222957276e-06),
        "embed_cols": jnp.clip(jnp.exp(jax.random.uniform(arg_keys[14], (EXTRA,), jnp.float32, math.log(2.6490953874969136e-09), math.log(2.6490952222957276e-06))), 2.6490953874969136e-09, 2.6490952222957276e-06),
        "head_weight": normal_values(arg_keys[15], (D, CLASSES), (D // 4) ** -0.5, 0.4375, ((0, 32),), jnp.float32),
        "head_rows": jnp.clip(jnp.exp(math.log(0.0015625) - 6.9077553 * jax.random.uniform(arg_keys[16], (D,), jnp.float32) ** block_scale(arg_keys[16], (D,), ((0, 32),), -0.2, 0.2)), 1.56249996052793e-06, 0.0015625),
        "head_cols": jnp.clip(jnp.exp(jax.random.uniform(arg_keys[17], (CLASSES,), jnp.float32, math.log(1.56249996052793e-06), math.log(0.0015625))), 1.56249996052793e-06, 0.0015625),
        "split_vec": normal_values(arg_keys[18], (LAYERS, 2, D), 0.3, 2.0, ((2, 4),), jnp.float32),
        "split_sq": jnp.clip(jnp.exp(math.log(0.00024414062) - 1.3862944 * jax.random.uniform(arg_keys[19], (LAYERS, 2, D), jnp.float32) ** block_scale(arg_keys[19], (LAYERS, 2, D), ((2, 4),), -0.2, 0.2)), 6.103515625e-05, 0.00024414062),
        "hidden_bias": normal_values(arg_keys[20], (LAYERS, FF), 0.3, 2.0, ((1, 4),), jnp.float32),
        "hidden_sq": jnp.clip(jnp.exp(math.log(0.00024414062) - 1.3862944 * jax.random.uniform(arg_keys[21], (LAYERS, FF), jnp.float32) ** block_scale(arg_keys[21], (LAYERS, FF), ((1, 4),), -0.2, 0.2)), 6.103515625e-05, 0.00024414062),
        "shared_vec": jnp.clip(1.0 + 0.15 * jax.random.normal(arg_keys[22], (6 * LAYERS + 2, D), jnp.float32), 0.25, 1.75),
        "shared_sq": jnp.clip(jnp.exp(jax.random.uniform(arg_keys[23], (6 * LAYERS + 2, D), jnp.float32, math.log(6.103515625e-05), math.log(0.00024414062))), 6.103515625e-05, 0.00024414062),
        "head_bias": normal_values(arg_keys[24], (CLASSES,), 0.5, 3.0, (), jnp.float32),
        "head_bias_sq": jnp.clip(jnp.exp(jax.random.uniform(arg_keys[25], (CLASSES,), jnp.float32, math.log(9.999999974752427e-07), math.log(3.999999989900971e-06))), 9.999999974752427e-07, 3.999999989900971e-06),
    }


decay_rate = 0.5
tiny_sq = 1e-30
floor_scale = 0.001
step_ratio = 1.0
clip_level = 0.1
smoothing = 0.1
norm_eps = 1e-06
highest = lax.Precision.HIGHEST

@jax.custom_vjp
def low(v):
    return lax.optimization_barrier(v.astype(jnp.bfloat16)).astype(jnp.float32)

@jax.custom_vjp
def low_back(v):
    return v

def low_keep(v):
    return (low(v), None)

def low_pass(kept, grad):
    return (grad,)

def back_keep(v):
    return (v, None)

def back_low(kept, grad):
    return (low(grad),)
low.defvjp(low_keep, low_pass)
low_back.defvjp(back_keep, back_low)

def layer_norm(values, gain_vec, shift_vec):
    centred = values - lax.optimization_barrier(jnp.mean(values, axis=-1, keepdims=True))
    spread = lax.optimization_barrier(jnp.mean(centred * centred, axis=-1, keepdims=True))
    return centred * lax.rsqrt(spread + norm_eps) * gain_vec + shift_vec

def product(left_side, right_side):
    return jnp.matmul(left_side, right_side, precision=highest)

def apply_update(weight, update, axes):
    clip_factor = jnp.maximum(1.0, jnp.sqrt(lax.optimization_barrier(jnp.mean(update * update, axis=axes, keepdims=True))) / clip_level)
    step_size = step_ratio * jnp.maximum(floor_scale, jnp.sqrt(lax.optimization_barrier(jnp.mean(weight * weight, axis=axes, keepdims=True))))
    return weight - step_size * update / clip_factor

def factored(weight, grad, row_stat, col_stat):
    grad_sq = grad * grad
    row_new = decay_rate * row_stat + (1.0 - decay_rate) * (lax.optimization_barrier(jnp.mean(grad_sq, axis=-1)) + tiny_sq)
    col_new = decay_rate * col_stat + (1.0 - decay_rate) * (lax.optimization_barrier(jnp.mean(grad_sq, axis=-2)) + tiny_sq)
    row_mean = lax.optimization_barrier(jnp.mean(row_new, axis=-1))
    second = row_new[..., :, None] * col_new[..., None, :] / row_mean[..., None, None]
    update = grad * lax.rsqrt(second)
    return (apply_update(weight, update, (-2, -1)), row_new, col_new)

def unfactored(weight, grad, second):
    second_new = decay_rate * second + (1.0 - decay_rate) * (grad * grad + tiny_sq)
    update = grad * lax.rsqrt(second_new)
    return (apply_update(weight, update, (-1,)), second_new)

def reference(patches, labels, image_count, attn_weight, attn_rows, attn_cols, mlp_weight, mlp_rows, mlp_cols, patch_weight, patch_rows, patch_cols, embed_table, embed_rows, embed_cols, head_weight, head_rows, head_cols, split_vec, split_sq, hidden_bias, hidden_sq, shared_vec, shared_sq, head_bias, head_bias_sq):
    patch_group = patches.astype(jnp.float32).reshape(N_DP, SLOTS, TOK_IMG - 1, PATCH)
    label_group = labels.reshape(N_DP, SLOTS)
    slot_index = jnp.arange(SLOTS)
    live = jnp.where(slot_index[None, :] < image_count[:, None], 1.0, 0.0).astype(jnp.float32)
    image_weight = live / jnp.sum(image_count).astype(jnp.float32)
    score_scale = HEAD_DIM ** (-0.5)
    key_valid = jnp.arange(SEQ) < TOK_IMG

    def forward(patch_w, embed_t, head_w, attn_w, mlp_w, split_v, hidden_b, shared_v, head_b):
        patch_lo = low(patch_w)
        table_rows = low(embed_t).T
        head_lo = low(head_w)
        attn_lo = low(attn_w)
        mlp_lo = low(mlp_w)

        def group_loss(carry, inputs):
            pixels, classes, weights = inputs
            embedded = low_back(product(pixels, patch_lo)) + table_rows[TOK_IMG] + table_rows[1:TOK_IMG]
            first_row = jnp.broadcast_to(table_rows[0], (SLOTS, 1, D))
            padding = jnp.zeros((SLOTS, SEQ - TOK_IMG, D), jnp.float32)
            residual = jnp.concatenate([first_row, embedded, padding], axis=1)
            head_shape = (SLOTS, SEQ, HEADS, HEAD_DIM)
            for layer_idx in range(LAYERS):
                gains = shared_v[6 * layer_idx:6 * layer_idx + 6]
                normed = low(layer_norm(residual, gains[0], gains[1]))
                query_heads = low(low_back(product(normed, attn_lo[layer_idx, :, 0])) + split_v[layer_idx, 0]).reshape(head_shape)
                key_heads = low(low_back(product(normed, attn_lo[layer_idx, :, 1]))).reshape(head_shape)
                value_heads = low(low_back(product(normed, attn_lo[layer_idx, :, 2])) + split_v[layer_idx, 1]).reshape(head_shape)
                raw_scores = jnp.einsum('bqhd,bkhd->bhqk', query_heads, key_heads, precision=highest)
                scores = jnp.where(key_valid, low_back(raw_scores) * score_scale, -1e+30)
                probs = jax.nn.softmax(scores, axis=-1)
                mixed = low(low_back(jnp.einsum('bhqk,bkhd->bqhd', low(probs), value_heads, precision=highest)))
                mixed = mixed.reshape(SLOTS, SEQ, D)
                residual = residual + low_back(product(mixed, attn_lo[layer_idx, :, 3].T)) + gains[2]
                mlp_in = low(layer_norm(residual, gains[3], gains[4]))
                hidden_pre = low_back(product(mlp_in, mlp_lo[layer_idx, 0])) + hidden_b[layer_idx]
                hidden_act = low(jax.nn.gelu(hidden_pre, approximate=False))
                residual = residual + low_back(product(hidden_act, mlp_lo[layer_idx, 1].T)) + gains[5]
            feature = low(layer_norm(residual[:, 0], shared_v[6 * LAYERS], shared_v[6 * LAYERS + 1]))
            logits = low_back(product(feature, head_lo)) + head_b
            onehot = jnp.where(classes[:, None] == jnp.arange(CLASSES)[None, :], 1.0, 0.0).astype(jnp.float32)
            target = (1.0 - smoothing) * onehot + smoothing / CLASSES
            entropy = jax.nn.logsumexp(logits, axis=-1) - lax.optimization_barrier(jnp.sum(target * logits, axis=-1))
            return (carry + jnp.sum(entropy * weights), None)
        total_loss, _ = lax.scan(jax.checkpoint(group_loss), jnp.zeros((), jnp.float32), (patch_group, label_group, image_weight))
        return total_loss
    mean_loss, pull = jax.vjp(forward, patch_weight, embed_table, head_weight, attn_weight, mlp_weight, split_vec, hidden_bias, shared_vec, head_bias)
    grad_patch, grad_table, grad_head, grad_attn, grad_mlp, grad_split, grad_hidden, grad_shared, grad_head_bias = pull(jnp.ones_like(mean_loss))
    attn_new, attn_rows_new, attn_cols_new = factored(attn_weight.transpose(0, 2, 1, 3), grad_attn.transpose(0, 2, 1, 3), attn_rows, attn_cols)
    attn_new = attn_new.transpose(0, 2, 1, 3)
    mlp_new, mlp_rows_new, mlp_cols_new = factored(mlp_weight, grad_mlp, mlp_rows, mlp_cols)
    patch_new, patch_rows_new, patch_cols_new = factored(patch_weight, grad_patch, patch_rows, patch_cols)
    embed_new, embed_rows_new, embed_cols_new = factored(embed_table, grad_table, embed_rows, embed_cols)
    head_new, head_rows_new, head_cols_new = factored(head_weight, grad_head, head_rows, head_cols)
    split_new, split_sq_new = unfactored(split_vec, grad_split, split_sq)
    hidden_new, hidden_sq_new = unfactored(hidden_bias, grad_hidden, hidden_sq)
    shared_new, shared_sq_new = unfactored(shared_vec, grad_shared, shared_sq)
    head_bias_new, head_bias_sq_new = unfactored(head_bias, grad_head_bias, head_bias_sq)
    return (mean_loss, attn_new, attn_rows_new, attn_cols_new, mlp_new, mlp_rows_new, mlp_cols_new, patch_new, patch_rows_new, patch_cols_new, embed_new, embed_rows_new, embed_cols_new, head_new, head_rows_new, head_cols_new, split_new, split_sq_new, hidden_new, hidden_sq_new, shared_new, shared_sq_new, head_bias_new, head_bias_sq_new)
```

```python
from functools import partial
import math

import jax
import jax.numpy as jnp
from jax import lax
from jax.sharding import PartitionSpec as P

D = 768
HEAD_DIM = 64
FF = 3072
PATCH = 768
CLASSES = 1000
TOK_IMG = 197
LAYERS = 3
SEQ = 200
EXTRA = 198


decay_rate = 0.5
tiny_sq = 1e-30
floor_scale = 0.001
step_ratio = 1.0
clip_level = 0.1
smoothing = 0.1
norm_eps = 1e-06


def layer_norm(values, gain_vec, shift_vec):
    centred = values - jnp.mean(values, axis=-1, keepdims=True)
    spread = jnp.mean(centred * centred, axis=-1, keepdims=True)
    return centred * lax.rsqrt(spread + norm_eps) * gain_vec + shift_vec


def outer_sum(left_rows, right_rows):
    return lax.dot_general(
        left_rows, right_rows, (((0,), (0,)), ((), ())), preferred_element_type=jnp.float32
    )


def times_transposed(left_rows, right_matrix):
    return lax.dot_general(
        left_rows, right_matrix, (((1,), (1,)), ((), ())), preferred_element_type=jnp.float32
    )


def flatten_all(arrays):
    return jnp.concatenate([jnp.ravel(member) for member in arrays])


def split_all(flat, shapes):
    outputs = []
    offset = 0
    for form_shape in shapes:
        length = math.prod(form_shape)
        outputs.append(flat[offset : offset + length].reshape(form_shape))
        offset = offset + length
    return outputs


def summed_over(axes, arrays):
    return split_all(
        lax.psum(flatten_all(arrays), axes), [member.shape for member in arrays]
    )


def gather_blocks(blocks):
    width = lax.axis_size("tensor")
    full = lax.all_gather(blocks, ("dp", "tensor"), axis=0, tiled=False)
    return full.reshape((-1, width) + blocks.shape)


def scatter_blocks(blocks):
    flat = blocks.reshape((-1,) + blocks.shape[2:])
    return lax.psum_scatter(flat, ("dp", "tensor"), scatter_dimension=0, tiled=False)


def finish_step(weight, update, update_sq, weight_sq, entries):
    clip_factor = jnp.maximum(1.0, jnp.sqrt(update_sq / entries) / clip_level)
    step_size = step_ratio * jnp.maximum(floor_scale, jnp.sqrt(weight_sq / entries))
    return weight - step_size * update / clip_factor


def shards(
    patches, labels, image_count,
    attn_weight, attn_rows, attn_cols,
    mlp_weight, mlp_rows, mlp_cols,
    patch_weight, patch_rows, patch_cols,
    embed_table, embed_rows, embed_cols,
    head_weight, head_rows, head_cols,
    split_vec, split_sq, hidden_bias, hidden_sq,
    shared_vec, shared_sq, head_bias, head_bias_sq,
):
    both = ("dp", "tensor")
    tensor_width = lax.axis_size("tensor")
    dp_width = lax.axis_size("dp")
    tensor_rank = lax.axis_index("tensor")
    shard_rank = lax.axis_index("dp")
    images = patches.shape[0]
    row_count = images * SEQ
    own_rows = attn_weight.shape[1]
    attn_width = attn_weight.shape[3]
    mlp_width = mlp_weight.shape[3]
    heads = D // HEAD_DIM
    score_scale = HEAD_DIM ** (-0.5)
    head_shape = (images, SEQ, heads, HEAD_DIM)
    key_valid = jnp.arange(SEQ) < TOK_IMG
    slot_index = tensor_rank * images + jnp.arange(images)
    image_total = jnp.sum(image_count).astype(jnp.float32)
    image_weight = (
        jnp.where(slot_index < image_count[shard_rank], 1.0, 0.0).astype(jnp.float32) / image_total
    )

    low = jnp.bfloat16
    small_full = gather_blocks(
        jnp.concatenate([patch_weight, embed_table], axis=1).astype(low)[None]
    ).reshape(D, D + EXTRA)
    patch_full, table_full = small_full[:, :D], small_full[:, D:]
    layers = []
    for layer_idx in range(LAYERS):
        attn_full = gather_blocks(
            attn_weight[layer_idx].astype(low).reshape(1, own_rows, 4 * attn_width)
        )
        mlp_full = gather_blocks(mlp_weight[layer_idx].astype(low))
        attn_full = (
            attn_full.reshape(dp_width, tensor_width, own_rows, 4, attn_width)
            .transpose(3, 0, 2, 1, 4)
            .reshape(4, D, D)
        )
        mlp_full = mlp_full.transpose(2, 0, 3, 1, 4).reshape(2, D, FF)
        layers.append((attn_full, mlp_full))
    head_full = gather_blocks(head_weight.astype(low)[None]).reshape(D, CLASSES)
    split_full, hidden_full = split_vec, hidden_bias
    vectors = flatten_all([split_vec, hidden_bias])
    vectors = lax.all_gather(vectors, "tensor", axis=0, tiled=False)
    split_full = (
        vectors[:, : split_vec.size]
        .reshape(tensor_width, LAYERS, 2, attn_width)
        .transpose(1, 2, 0, 3)
        .reshape(LAYERS, 2, D)
    )
    hidden_full = (
        vectors[:, split_vec.size :]
        .reshape(tensor_width, LAYERS, mlp_width)
        .transpose(1, 0, 2)
        .reshape(LAYERS, FF)
    )

    table_rows = table_full.astype(jnp.float32).T
    pixel_rows = patches.reshape(images * (TOK_IMG - 1), PATCH)
    embedded = jnp.dot(pixel_rows, patch_full, preferred_element_type=jnp.float32).reshape(
        images, TOK_IMG - 1, D
    )
    embedded = embedded + table_rows[1:TOK_IMG] + table_rows[TOK_IMG]
    residual = jnp.concatenate(
        [
            jnp.broadcast_to(table_rows[0], (images, 1, D)),
            embedded,
            jnp.zeros((images, SEQ - TOK_IMG, D), jnp.float32),
        ],
        axis=1,
    ).reshape(row_count, D)

    def attend(query_heads, key_heads):
        scores = (
            jnp.einsum(
                "bqhd,bkhd->bhqk", query_heads, key_heads, preferred_element_type=jnp.float32
            )
            * score_scale
        )
        return jnp.where(key_valid, scores, -1e30)

    saved = []
    for layer_idx in range(LAYERS):
        attn_full, mlp_full = layers[layer_idx]
        gains = shared_vec[6 * layer_idx : 6 * layer_idx + 6]
        attn_input = residual
        normed = layer_norm(residual, gains[0], gains[1]).astype(low)
        query_rows = (
            jnp.dot(normed, attn_full[0], preferred_element_type=jnp.float32)
            + split_full[layer_idx, 0]
        ).astype(low)
        key_rows = jnp.dot(normed, attn_full[1], preferred_element_type=jnp.float32).astype(low)
        value_rows = (
            jnp.dot(normed, attn_full[2], preferred_element_type=jnp.float32)
            + split_full[layer_idx, 1]
        ).astype(low)
        scores = attend(query_rows.reshape(head_shape), key_rows.reshape(head_shape))
        log_total = jax.nn.logsumexp(scores, axis=-1, keepdims=True)
        probs = jnp.exp(scores - log_total)
        mixed = (
            jnp.einsum(
                "bhqk,bkhd->bqhd",
                probs.astype(low),
                value_rows.reshape(head_shape),
                preferred_element_type=jnp.float32,
            )
            .astype(low)
            .reshape(row_count, D)
        )
        residual = residual + times_transposed(mixed, attn_full[3]) + gains[2]
        mlp_input = residual
        mlp_normed = layer_norm(residual, gains[3], gains[4]).astype(low)
        hidden_pre = (
            jnp.dot(mlp_normed, mlp_full[0], preferred_element_type=jnp.float32)
            + hidden_full[layer_idx]
        )
        hidden_act = jax.nn.gelu(hidden_pre, approximate=False).astype(low)
        residual = residual + times_transposed(hidden_act, mlp_full[1]) + gains[5]
        saved.append(
            (
                attn_input, normed, query_rows, key_rows, value_rows, log_total,
                mixed, mlp_input, mlp_normed, hidden_pre, hidden_act,
            )
        )
    cls_rows = residual.reshape(images, SEQ, D)[:, 0]
    feature, final_back = jax.vjp(
        layer_norm, cls_rows, shared_vec[6 * LAYERS], shared_vec[6 * LAYERS + 1]
    )
    feature_low = feature.astype(low)
    logits = jnp.dot(feature_low, head_full, preferred_element_type=jnp.float32) + head_bias
    log_norm = jax.nn.logsumexp(logits, axis=-1, keepdims=True)
    onehot = jnp.where(labels[:, None] == jnp.arange(CLASSES)[None, :], 1.0, 0.0).astype(
        jnp.float32
    )
    target = (1.0 - smoothing) * onehot + smoothing / CLASSES
    loss_part = jnp.sum((log_norm[:, 0] - jnp.sum(target * logits, axis=-1)) * image_weight)
    grad_logits = (jnp.exp(logits - log_norm) - target) * image_weight[:, None]
    grad_head_bias = jnp.sum(grad_logits, axis=0)
    logits_low = grad_logits.astype(low)
    grad_head = outer_sum(feature_low, logits_low)
    grad_feature = times_transposed(logits_low, head_full)
    grad_cls, grad_final_gain, grad_final_shift = final_back(grad_feature)
    grad_rows = jnp.concatenate(
        [grad_cls[:, None], jnp.zeros((images, SEQ - 1, D), jnp.float32)], axis=1
    ).reshape(row_count, D)
    head_grad = scatter_blocks(
        grad_head.astype(low).reshape(dp_width, tensor_width, 1, -1, CLASSES)
    )[0].astype(jnp.float32)
    shared_list = [None] * LAYERS
    split_list = [None] * LAYERS
    hidden_list = [None] * LAYERS
    attn_list = [None] * LAYERS
    mlp_list = [None] * LAYERS
    for layer_idx in reversed(range(LAYERS)):
        (
            attn_input, normed, query_rows, key_rows, value_rows, log_total,
            mixed, mlp_input, mlp_normed, hidden_pre, hidden_act,
        ) = saved[layer_idx]
        attn_full, mlp_full = layers[layer_idx]
        gains = shared_vec[6 * layer_idx : 6 * layer_idx + 6]
        grad_down_bias = jnp.sum(grad_rows, axis=0)
        grad_out = grad_rows.astype(low)
        grad_act = jnp.dot(grad_out, mlp_full[1], preferred_element_type=jnp.float32)
        grad_down = outer_sum(grad_out, hidden_act)
        _, gelu_back = jax.vjp(partial(jax.nn.gelu, approximate=False), hidden_pre)
        grad_pre = gelu_back(grad_act)[0]
        hidden_list[layer_idx] = jnp.sum(grad_pre, axis=0)
        pre_low = grad_pre.astype(low)
        grad_up = outer_sum(mlp_normed, pre_low)
        mlp_blocks = (
            jnp.stack([grad_up.astype(low), grad_down.astype(low)])
            .reshape(2, dp_width, own_rows, tensor_width, mlp_width)
            .transpose(1, 3, 0, 2, 4)
        )
        mlp_list[layer_idx] = scatter_blocks(mlp_blocks).astype(jnp.float32)
        grad_mlp_in = times_transposed(pre_low, mlp_full[0])
        _, second_back = jax.vjp(layer_norm, mlp_input, gains[3], gains[4])
        grad_mid, grad_gain_two, grad_shift_two = second_back(grad_mlp_in)
        grad_rows = grad_rows + grad_mid
        grad_out_bias = jnp.sum(grad_rows, axis=0)
        grad_attn_out = grad_rows.astype(low)
        grad_mixed = (
            jnp.dot(grad_attn_out, attn_full[3], preferred_element_type=jnp.float32)
            .astype(low)
            .reshape(head_shape)
        )
        grad_out_proj = outer_sum(grad_attn_out, mixed)
        query_heads = query_rows.reshape(head_shape)
        key_heads = key_rows.reshape(head_shape)
        value_heads = value_rows.reshape(head_shape)
        probs = jnp.exp(attend(query_heads, key_heads) - log_total)
        grad_probs = jnp.einsum(
            "bqhd,bkhd->bhqk", grad_mixed, value_heads, preferred_element_type=jnp.float32
        )
        grad_value = jnp.einsum(
            "bhqk,bqhd->bkhd", probs.astype(low), grad_mixed, preferred_element_type=jnp.float32
        ).reshape(row_count, D)
        inner_sum = jnp.sum(probs * grad_probs, axis=-1, keepdims=True)
        grad_scores = (probs * (grad_probs - inner_sum) * score_scale).astype(low)
        grad_query = jnp.einsum(
            "bhqk,bkhd->bqhd", grad_scores, key_heads, preferred_element_type=jnp.float32
        ).reshape(row_count, D)
        grad_key = jnp.einsum(
            "bhqk,bqhd->bkhd", grad_scores, query_heads, preferred_element_type=jnp.float32
        ).reshape(row_count, D)
        split_list[layer_idx] = jnp.stack([jnp.sum(grad_query, axis=0), jnp.sum(grad_value, axis=0)])
        query_low, key_low, value_low = (
            grad_query.astype(low), grad_key.astype(low), grad_value.astype(low)
        )
        attn_blocks = (
            jnp.stack(
                [
                    outer_sum(normed, query_low).astype(low),
                    outer_sum(normed, key_low).astype(low),
                    outer_sum(normed, value_low).astype(low),
                    grad_out_proj.astype(low),
                ]
            )
            .reshape(4, dp_width, own_rows, tensor_width, attn_width)
            .transpose(1, 3, 2, 0, 4)
            .reshape(dp_width, tensor_width, 1, own_rows, 4 * attn_width)
        )
        attn_list[layer_idx] = (
            scatter_blocks(attn_blocks).astype(jnp.float32).reshape(own_rows, 4, attn_width)
        )
        grad_attn_in = (
            times_transposed(query_low, attn_full[0])
            + times_transposed(key_low, attn_full[1])
            + times_transposed(value_low, attn_full[2])
        )
        _, first_back = jax.vjp(layer_norm, attn_input, gains[0], gains[1])
        grad_low, grad_gain_one, grad_shift_one = first_back(grad_attn_in)
        grad_rows = grad_rows + grad_low
        shared_list[layer_idx] = jnp.stack(
            [
                grad_gain_one, grad_shift_one, grad_out_bias,
                grad_gain_two, grad_shift_two, grad_down_bias,
            ]
        )
    grad_image = grad_rows.reshape(images, SEQ, D)
    grad_first = jnp.sum(grad_image[:, 0], axis=0)
    grad_position = jnp.sum(grad_image[:, 1:TOK_IMG], axis=0)
    grad_patch_bias = jnp.sum(grad_position, axis=0)
    embed_low = grad_image[:, 1:TOK_IMG].astype(low).reshape(images * (TOK_IMG - 1), D)
    grad_patch = outer_sum(pixel_rows, embed_low)
    grad_table = jnp.concatenate([grad_first[None], grad_position, grad_patch_bias[None]], axis=0).T
    small_grad = scatter_blocks(
        jnp.concatenate([grad_patch, grad_table], axis=1)
        .astype(low)
        .reshape(dp_width, tensor_width, 1, -1, D + EXTRA)
    )[0].astype(jnp.float32)
    patch_grad, table_grad = small_grad[:, :D], small_grad[:, D:]
    attn_grad = jnp.stack(attn_list)
    mlp_grad = jnp.stack(mlp_list)
    shared_grad = jnp.concatenate(
        shared_list + [jnp.stack([grad_final_gain, grad_final_shift])], axis=0
    )
    attn_sq = attn_grad * attn_grad
    mlp_sq = mlp_grad * mlp_grad
    patch_sq = patch_grad * patch_grad
    table_sq = table_grad * table_grad
    head_sq = head_grad * head_grad

    split_sums, hidden_sums, shared_full, head_bias_full, loss_total = summed_over(
        both, [jnp.stack(split_list), jnp.stack(hidden_list), shared_grad, grad_head_bias, loss_part]
    )
    split_total = lax.dynamic_slice_in_dim(split_sums, tensor_rank * attn_width, attn_width, 2)
    hidden_total = lax.dynamic_slice_in_dim(hidden_sums, tensor_rank * mlp_width, mlp_width, 1)
    attn_row_full, mlp_row_full = summed_over(
        "tensor", [jnp.sum(attn_sq, axis=3).transpose(0, 2, 1), jnp.sum(mlp_sq, axis=3)]
    )
    attn_col_full, mlp_col_full = summed_over("dp", [jnp.sum(attn_sq, axis=1), jnp.sum(mlp_sq, axis=2)])
    attn_row_new = decay_rate * attn_rows + (1.0 - decay_rate) * (attn_row_full / D + tiny_sq)
    mlp_row_new = decay_rate * mlp_rows + (1.0 - decay_rate) * (mlp_row_full / FF + tiny_sq)
    patch_row_new = decay_rate * patch_rows + (1.0 - decay_rate) * (
        jnp.sum(patch_sq, axis=1) / D + tiny_sq
    )
    table_row_new = decay_rate * embed_rows + (1.0 - decay_rate) * (
        jnp.sum(table_sq, axis=1) / EXTRA + tiny_sq
    )
    head_row_new = decay_rate * head_rows + (1.0 - decay_rate) * (
        jnp.sum(head_sq, axis=1) / CLASSES + tiny_sq
    )
    own_share = 1.0 / tensor_width
    (
        patch_col_full, table_col_full, head_col_full, whole_row_sum,
        attn_old_sum, mlp_old_sum, attn_total, mlp_total, weight_sq_parts,
    ) = summed_over(
        both,
        [
            jnp.sum(patch_sq, axis=0),
            jnp.sum(table_sq, axis=0),
            jnp.sum(head_sq, axis=0),
            jnp.stack([jnp.sum(patch_row_new), jnp.sum(table_row_new), jnp.sum(head_row_new)]),
            jnp.sum(attn_rows, axis=-1) * own_share,
            jnp.sum(mlp_rows, axis=-1) * own_share,
            jnp.sum(attn_sq, axis=(1, 3)),
            jnp.sum(mlp_sq, axis=(2, 3)),
            flatten_all(
                [
                    jnp.sum(attn_weight * attn_weight, axis=(1, 3)),
                    jnp.sum(mlp_weight * mlp_weight, axis=(2, 3)),
                    jnp.sum(patch_weight * patch_weight),
                    jnp.sum(embed_table * embed_table),
                    jnp.sum(head_weight * head_weight),
                ]
            ),
        ],
    )
    weight_sq = split_all(weight_sq_parts, [(LAYERS, 4), (LAYERS, 2), (), (), ()])
    attn_row_mean = (
        decay_rate * attn_old_sum + (1.0 - decay_rate) * (attn_total / D + D * tiny_sq)
    ) / D
    mlp_row_mean = (
        decay_rate * mlp_old_sum + (1.0 - decay_rate) * (mlp_total / FF + D * tiny_sq)
    ) / D
    whole_row_mean = whole_row_sum / jnp.array([PATCH, D, D], jnp.float32)
    attn_col_new = decay_rate * attn_cols + (1.0 - decay_rate) * (attn_col_full / D + tiny_sq)
    mlp_col_new = decay_rate * mlp_cols + (1.0 - decay_rate) * (mlp_col_full / D + tiny_sq)
    patch_col_new = decay_rate * patch_cols + (1.0 - decay_rate) * (
        patch_col_full / PATCH + tiny_sq
    )
    table_col_new = decay_rate * embed_cols + (1.0 - decay_rate) * (table_col_full / D + tiny_sq)
    head_col_new = decay_rate * head_cols + (1.0 - decay_rate) * (head_col_full / D + tiny_sq)
    attn_update = attn_grad * lax.rsqrt(
        attn_row_new.transpose(0, 2, 1)[:, :, :, None]
        * attn_col_new[:, None]
        / attn_row_mean[:, None, :, None]
    )
    mlp_update = mlp_grad * lax.rsqrt(
        mlp_row_new[:, :, :, None] * mlp_col_new[:, :, None, :] / mlp_row_mean[:, :, None, None]
    )
    patch_update = patch_grad * lax.rsqrt(
        patch_row_new[:, None] * patch_col_new[None, :] / whole_row_mean[0]
    )
    table_update = table_grad * lax.rsqrt(
        table_row_new[:, None] * table_col_new[None, :] / whole_row_mean[1]
    )
    head_update = head_grad * lax.rsqrt(
        head_row_new[:, None] * head_col_new[None, :] / whole_row_mean[2]
    )
    split_sq_new = decay_rate * split_sq + (1.0 - decay_rate) * (
        split_total * split_total + tiny_sq
    )
    split_update = split_total * lax.rsqrt(split_sq_new)
    hidden_sq_new = decay_rate * hidden_sq + (1.0 - decay_rate) * (
        hidden_total * hidden_total + tiny_sq
    )
    hidden_update = hidden_total * lax.rsqrt(hidden_sq_new)
    shared_sq_new = decay_rate * shared_sq + (1.0 - decay_rate) * (
        shared_full * shared_full + tiny_sq
    )
    shared_update = shared_full * lax.rsqrt(shared_sq_new)
    head_bias_sq_new = decay_rate * head_bias_sq + (1.0 - decay_rate) * (
        head_bias_full * head_bias_full + tiny_sq
    )
    head_bias_update = head_bias_full * lax.rsqrt(head_bias_sq_new)
    dp_share = 1.0 / dp_width
    attn_u2, mlp_u2, patch_u2, table_u2, head_u2, split_u2, hidden_u2, split_w2, hidden_w2 = (
        summed_over(
            both,
            [
                jnp.sum(attn_update * attn_update, axis=(1, 3)),
                jnp.sum(mlp_update * mlp_update, axis=(2, 3)),
                jnp.sum(patch_update * patch_update),
                jnp.sum(table_update * table_update),
                jnp.sum(head_update * head_update),
                jnp.sum(split_update * split_update, axis=-1) * dp_share,
                jnp.sum(hidden_update * hidden_update, axis=-1) * dp_share,
                jnp.sum(split_vec * split_vec, axis=-1) * dp_share,
                jnp.sum(hidden_bias * hidden_bias, axis=-1) * dp_share,
            ],
        )
    )
    vector_sq = [split_w2, hidden_w2]
    attn_new = finish_step(
        attn_weight, attn_update, attn_u2[:, None, :, None], weight_sq[0][:, None, :, None], D * D
    )
    mlp_new = finish_step(
        mlp_weight, mlp_update, mlp_u2[:, :, None, None], weight_sq[1][:, :, None, None], D * FF
    )
    patch_new = finish_step(patch_weight, patch_update, patch_u2, weight_sq[2], PATCH * D)
    embed_new = finish_step(embed_table, table_update, table_u2, weight_sq[3], D * EXTRA)
    head_new = finish_step(head_weight, head_update, head_u2, weight_sq[4], D * CLASSES)
    split_new = finish_step(
        split_vec, split_update, split_u2[:, :, None], vector_sq[0][:, :, None], D
    )
    hidden_new = finish_step(
        hidden_bias, hidden_update, hidden_u2[:, None], vector_sq[1][:, None], FF
    )
    shared_new = finish_step(
        shared_vec,
        shared_update,
        jnp.sum(shared_update * shared_update, axis=-1, keepdims=True),
        jnp.sum(shared_vec * shared_vec, axis=-1, keepdims=True),
        D,
    )
    head_bias_new = finish_step(
        head_bias,
        head_bias_update,
        jnp.sum(head_bias_update * head_bias_update),
        jnp.sum(head_bias * head_bias),
        CLASSES,
    )
    return (
        loss_total,
        attn_new,
        attn_row_new,
        attn_col_new,
        mlp_new,
        mlp_row_new,
        mlp_col_new,
        patch_new,
        patch_row_new,
        patch_col_new,
        embed_new,
        table_row_new,
        table_col_new,
        head_new,
        head_row_new,
        head_col_new,
        split_new,
        split_sq_new,
        hidden_new,
        hidden_sq_new,
        shared_new,
        shared_sq_new,
        head_bias_new,
        head_bias_sq_new,
    )


def solution(mesh):
    in_specs = (
        P(("dp", "tensor"), None, None),
        P(("dp", "tensor")),
        P(),
        P(None, "dp", None, "tensor"),
        P(None, None, "dp"),
        P(None, None, "tensor"),
        P(None, None, "dp", "tensor"),
        P(None, None, "dp"),
        P(None, None, "tensor"),
        P(("dp", "tensor"), None),
        P(("dp", "tensor")),
        P(),
        P(("dp", "tensor"), None),
        P(("dp", "tensor")),
        P(),
        P(("dp", "tensor"), None),
        P(("dp", "tensor")),
        P(),
        P(None, None, "tensor"),
        P(None, None, "tensor"),
        P(None, "tensor"),
        P(None, "tensor"),
        P(),
        P(),
        P(),
        P(),
    )
    out_specs = (
        P(),
        P(None, "dp", None, "tensor"),
        P(None, None, "dp"),
        P(None, None, "tensor"),
        P(None, None, "dp", "tensor"),
        P(None, None, "dp"),
        P(None, None, "tensor"),
        P(("dp", "tensor"), None),
        P(("dp", "tensor")),
        P(),
        P(("dp", "tensor"), None),
        P(("dp", "tensor")),
        P(),
        P(("dp", "tensor"), None),
        P(("dp", "tensor")),
        P(),
        P(None, None, "tensor"),
        P(None, None, "tensor"),
        P(None, "tensor"),
        P(None, "tensor"),
        P(),
        P(),
        P(),
        P(),
    )
    return jax.shard_map(shards, mesh=mesh, in_specs=in_specs, out_specs=out_specs, check_vma=False)
```

```python
from functools import partial
import math

import jax
import jax.numpy as jnp
from jax import lax
from jax.experimental import pallas as pl
from jax.experimental.pallas import tpu as pltpu
from jax.sharding import PartitionSpec as P

D = 768
HEAD_DIM = 64
FF = 3072
PATCH = 768
CLASSES = 1000
TOK_IMG = 197
LAYERS = 3
SEQ = 200
EXTRA = 198


decay_rate = 0.5
tiny_sq = 1e-30
floor_scale = 0.001
step_ratio = 1.0
clip_level = 0.1
smoothing = 0.1
norm_eps = 1e-06


def layer_norm(values, gain_vec, shift_vec):
    centred = values - jnp.mean(values, axis=-1, keepdims=True)
    spread = jnp.mean(centred * centred, axis=-1, keepdims=True)
    return centred * lax.rsqrt(spread + norm_eps) * gain_vec + shift_vec


def outer_sum(left_rows, right_rows):
    return lax.dot_general(
        left_rows, right_rows, (((0,), (0,)), ((), ())), preferred_element_type=jnp.float32
    )


def times_transposed(left_rows, right_matrix):
    return lax.dot_general(
        left_rows, right_matrix, (((1,), (1,)), ((), ())), preferred_element_type=jnp.float32
    )


def flatten_all(arrays):
    return jnp.concatenate([jnp.ravel(member) for member in arrays])


def split_all(flat, shapes):
    outputs = []
    offset = 0
    for form_shape in shapes:
        length = math.prod(form_shape)
        outputs.append(flat[offset : offset + length].reshape(form_shape))
        offset = offset + length
    return outputs


def summed_over(axes, arrays):
    return split_all(
        lax.psum(flatten_all(arrays), axes), [member.shape for member in arrays]
    )


MESH = pl.DeviceIdType.MESH
DIMS = ("y", "c", "zb", "za", "x")
OUT_ORDERS = (("zb", "za", "x", "y", "c"), ("zb", "za", "y", "x", "c"))
IN_ORDERS = (("c", "y", "x", "za", "zb"), ("c", "x", "y", "za", "zb"))


def place_of_device():
    dp, tensor = lax.axis_index("dp"), lax.axis_index("tensor")
    return {
        "x": lax.rem(dp, 2),
        "za": lax.rem(dp // 2, 2),
        "zb": dp // 4,
        "y": tensor // 2,
        "c": lax.rem(tensor, 2),
    }


def partner_of(place, dim):
    moved = dict(place)
    moved[dim] = 1 - place[dim]
    return (
        moved["zb"] * 4 + moved["za"] * 2 + moved["x"],
        moved["y"] * 2 + moved["c"],
    )


def meet_partners(place):
    barrier = pltpu.get_barrier_semaphore()
    for dim in DIMS:
        pl.semaphore_signal(
            barrier, inc=1, device_id=partner_of(place, dim), device_id_type=MESH
        )
    pl.semaphore_wait(barrier, len(DIMS))


def spread_kernel(groups, *refs):
    arrays = len({flow[0] for group in groups for flow in group})
    sources, targets = refs[:arrays], refs[arrays : 2 * arrays]
    send_sem, recv_sem, own_sem = refs[2 * arrays :]
    place = place_of_device()
    flows = [flow for group in groups for flow in group]
    number = {flow: position for position, flow in enumerate(flows)}

    def own_copy(flow):
        array, lead, tail, _ = flow
        slot = lead + tuple(place[dim] for dim in DIMS) + tail
        return pltpu.make_async_copy(
            sources[array].at[lead + tail], targets[array].at[slot], own_sem.at[number[flow]]
        )

    def stage_copy(flow, stage):
        array, lead, tail, order = flow
        dims = OUT_ORDERS[order]
        done = dims[:stage]
        slot = lead + tuple(slice(None) if dim in done else place[dim] for dim in DIMS) + tail
        source = sources[array].at[lead + tail] if stage == 0 else targets[array].at[slot]
        return pltpu.make_async_remote_copy(
            src_ref=source,
            dst_ref=targets[array].at[slot],
            send_sem=send_sem.at[number[flow], stage],
            recv_sem=recv_sem.at[number[flow], stage],
            device_id=partner_of(place, dims[stage]),
            device_id_type=MESH,
        )

    meet_partners(place)
    stages = len(DIMS)
    for tick in range(len(groups) + stages):
        for stage in reversed(range(stages + 1)):
            if not 0 <= tick - stage < len(groups):
                continue
            for flow in groups[tick - stage]:
                if stage == 1:
                    own_copy(flow).wait()
                if stage > 0:
                    stage_copy(flow, stage - 1).wait_recv()
                if stage == 0:
                    own_copy(flow).start()
                if stage < stages:
                    stage_copy(flow, stage).start()
    for flow in flows:
        for stage in range(stages):
            stage_copy(flow, stage).wait_send()


def spread(arrays, groups, collective_id):
    count = sum(len(group) for group in groups)
    leads = {flow[0]: len(flow[1]) for group in groups for flow in group}
    shapes = [
        member.shape[: leads[position]] + (2,) * len(DIMS) + member.shape[leads[position] :]
        for position, member in enumerate(arrays)
    ]
    return pl.pallas_call(
        partial(spread_kernel, groups),
        out_shape=[
            jax.ShapeDtypeStruct(shape, member.dtype) for shape, member in zip(shapes, arrays)
        ],
        in_specs=[pl.BlockSpec(memory_space=pltpu.VMEM)] * len(arrays),
        out_specs=[pl.BlockSpec(memory_space=pl.ANY)] * len(arrays),
        scratch_shapes=[
            pltpu.SemaphoreType.DMA((count, len(DIMS))),
            pltpu.SemaphoreType.DMA((count, len(DIMS))),
            pltpu.SemaphoreType.DMA((count,)),
        ],
        compiler_params=pltpu.CompilerParams(
            collective_id=collective_id, has_side_effects=True, vmem_limit_bytes=16 << 20
        ),
    )(*arrays)


def collect_kernel(groups, arrays, *refs):
    sources, targets = refs[:arrays], refs[arrays : 2 * arrays]
    held, landed = refs[2 * arrays], refs[2 * arrays + 1 : 2 * arrays + 6]
    send_sem, recv_sem, own_sem = refs[2 * arrays + 6 :]
    place = place_of_device()
    flows = [flow for group in groups for flow in group]
    number = {flow: position for position, flow in enumerate(flows)}
    kept = ("y", "zb", "za", "x")

    def core_slot(flow, core):
        _, lead, tail, _ = flow
        return lead + tuple(core if dim == "c" else slice(None) for dim in DIMS) + tail

    def own_copy(flow):
        return pltpu.make_async_copy(
            sources[flow[0]].at[core_slot(flow, place["c"])],
            held.at[number[flow]],
            own_sem.at[number[flow]],
        )

    def held_slot(done, moved):
        slot = ()
        for dim in kept:
            if dim == moved:
                slot += (1 - place[dim],)
            elif dim in done:
                slot += (place[dim],)
            else:
                slot += (slice(None),)
        return slot

    def stage_copy(flow, stage):
        dims = IN_ORDERS[flow[3]]
        index = number[flow]
        if stage == 0:
            source = sources[flow[0]].at[core_slot(flow, 1 - place["c"])]
        else:
            source = held.at[(index,) + held_slot(dims[:stage], dims[stage])]
        return pltpu.make_async_remote_copy(
            src_ref=source,
            dst_ref=landed[stage].at[index],
            send_sem=send_sem.at[index, stage],
            recv_sem=recv_sem.at[index, stage],
            device_id=partner_of(place, dims[stage]),
            device_id_type=MESH,
        )

    def add_landed(flow, stage):
        array, lead, tail, order = flow
        dims = IN_ORDERS[order]
        index = number[flow]
        free = [dim for dim in kept if dim not in dims[: stage + 1]]

        def add_block(step, carry):
            rest = step
            at = {}
            for dim in reversed(free):
                at[dim] = lax.rem(rest, 2)
                rest = rest // 2
            slot = (index,) + tuple(at[dim] if dim in free else place[dim] for dim in kept)
            landed_slot = (index,) + tuple(at[dim] for dim in free)
            total = held[slot].astype(jnp.float32) + landed[stage][landed_slot].astype(jnp.float32)
            if stage == len(DIMS) - 1:
                targets[array][lead + tail] = total
            else:
                held[slot] = total.astype(jnp.bfloat16)
            return carry

        if free:
            lax.fori_loop(0, 2 ** len(free), add_block, 0)
        else:
            add_block(0, 0)

    meet_partners(place)
    stages = len(DIMS)
    for tick in range(len(groups) + stages):
        for stage in reversed(range(stages + 1)):
            if not 0 <= tick - stage < len(groups):
                continue
            for flow in groups[tick - stage]:
                if stage == 0:
                    own_copy(flow).start()
                if stage == 1:
                    own_copy(flow).wait()
                if stage > 0:
                    stage_copy(flow, stage - 1).wait_recv()
                    add_landed(flow, stage - 1)
                if stage < stages:
                    stage_copy(flow, stage).start()
    for flow in flows:
        for stage in range(stages):
            stage_copy(flow, stage).wait_send()


def collect(arrays, groups, collective_id):
    leads = {flow[0]: len(flow[1]) for group in groups for flow in group}
    count = sum(len(group) for group in groups)
    block = arrays[0].shape[-2:]
    low = jnp.bfloat16
    return pl.pallas_call(
        partial(collect_kernel, groups, len(arrays)),
        out_shape=[
            jax.ShapeDtypeStruct(
                member.shape[: leads[position]] + member.shape[leads[position] + len(DIMS) :],
                jnp.float32,
            )
            for position, member in enumerate(arrays)
        ],
        in_specs=[pl.BlockSpec(memory_space=pl.ANY)] * len(arrays),
        out_specs=[pl.BlockSpec(memory_space=pltpu.VMEM)] * len(arrays),
        scratch_shapes=[
            pltpu.VMEM((count, 2, 2, 2, 2) + block, low),
            pltpu.VMEM((count, 2, 2, 2, 2) + block, low),
            pltpu.VMEM((count, 2, 2, 2) + block, low),
            pltpu.VMEM((count, 2, 2) + block, low),
            pltpu.VMEM((count, 2) + block, low),
            pltpu.VMEM((count,) + block, low),
            pltpu.SemaphoreType.DMA((count, len(DIMS))),
            pltpu.SemaphoreType.DMA((count, len(DIMS))),
            pltpu.SemaphoreType.DMA((count,)),
        ],
        compiler_params=pltpu.CompilerParams(
            collective_id=collective_id, has_side_effects=True, vmem_limit_bytes=48 << 20
        ),
    )(*arrays)


PAD_ROWS = 208
HALF_ROOT = 0.7071067811865476
DENSITY = 0.3989422804014327


def dot_nn(left, right):
    return lax.dot_general(left, right, (((1,), (0,)), ((), ())), preferred_element_type=jnp.float32)


def dot_nt(left, right):
    return lax.dot_general(left, right, (((1,), (1,)), ((), ())), preferred_element_type=jnp.float32)


def dot_tn(left, right):
    return lax.dot_general(left, right, (((0,), (0,)), ((), ())), preferred_element_type=jnp.float32)


def normal_form(values):
    centred = values - jnp.mean(values, axis=-1, keepdims=True)
    spread_sq = jnp.mean(centred * centred, axis=-1, keepdims=True)
    inverse = lax.rsqrt(spread_sq + norm_eps)
    return centred * inverse, inverse


def norm_back(grad, unit, inverse, gain):
    inner = grad * gain
    return inverse * (
        inner
        - jnp.mean(inner, axis=-1, keepdims=True)
        - unit * jnp.mean(inner * unit, axis=-1, keepdims=True)
    )


def head_probs(query, key):
    scores = dot_nt(query, key) * HEAD_DIM ** (-0.5)
    column = lax.broadcasted_iota(jnp.int32, scores.shape, 1)
    scores = jnp.where(column < TOK_IMG, scores, -1e30)
    powers = jnp.exp(scores - jnp.max(scores, axis=-1, keepdims=True))
    return powers / jnp.sum(powers, axis=-1, keepdims=True)


def forward_kernel(
    images, parts, x_ref, gain_ref, attn_ref, up_ref, down_ref, split_ref, hidden_ref,
    next_ref, mid_ref, qkv_ref, mixed_ref, act_ref, slope_ref, normed,
):
    step = pl.program_id(0)
    low = jnp.bfloat16
    width = mixed_ref.shape[-1]
    heads = width // HEAD_DIM

    @pl.when(step == 0)
    def _():
        unit, _ = normal_form(x_ref[...])
        normed[...] = (unit * gain_ref[0:1] + gain_ref[1:2]).astype(low)
        mid_ref[...] = x_ref[...] + gain_ref[2:3]

    @pl.when(step < parts)
    def _():
        weights = attn_ref[0]
        qkv = (dot_nn(normed[...], weights[:, : 3 * width]) + split_ref[0]).astype(low)
        qkv_ref[0] = qkv
        columns = []
        for head in range(heads):
            rows = []
            for image in range(images):
                at = slice(image * PAD_ROWS, (image + 1) * PAD_ROWS)
                query, key, value = (
                    qkv[at, kind * width + head * HEAD_DIM : kind * width + (head + 1) * HEAD_DIM]
                    for kind in range(3)
                )
                probs = head_probs(query, key).astype(low)
                rows.append(dot_nn(probs, value).astype(low))
            columns.append(jnp.concatenate(rows, axis=0))
        mixed = jnp.concatenate(columns, axis=1)
        mixed_ref[0] = mixed
        mid_ref[...] += dot_nt(mixed, weights[:, 3 * width :])

    @pl.when(step == parts)
    def _():
        unit, _ = normal_form(mid_ref[...])
        normed[...] = (unit * gain_ref[3:4] + gain_ref[4:5]).astype(low)
        next_ref[...] = mid_ref[...] + gain_ref[5:6]

    @pl.when(step >= parts)
    def _():
        pre = dot_nn(normed[...], up_ref[0]) + hidden_ref[0]
        share = 0.5 * (1.0 + lax.erf(pre * HALF_ROOT))
        act = (pre * share).astype(low)
        act_ref[0] = act
        slope_ref[0] = (share + pre * (DENSITY * jnp.exp(-0.5 * pre * pre))).astype(low)
        next_ref[...] += dot_nt(act, down_ref[0])


def forward_layer(layer_idx, images, x, gains, weights, split_rows, hidden_rows):
    rows = x.shape[0]
    parts = hidden_rows.shape[0]
    base = layer_idx * 3 * parts
    width, hidden = split_rows.shape[-1] // 3, hidden_rows.shape[-1]
    block = weights.shape[1:]
    early = lambda step: jnp.minimum(step, parts - 1)
    late = lambda step: jnp.maximum(step - parts, 0)
    whole = lambda shape: pl.BlockSpec(shape, lambda step: (0,) * len(shape))
    low = jnp.bfloat16
    return pl.pallas_call(
        partial(forward_kernel, images, parts),
        grid=(2 * parts,),
        out_shape=[
            jax.ShapeDtypeStruct((rows, D), jnp.float32),
            jax.ShapeDtypeStruct((rows, D), jnp.float32),
            jax.ShapeDtypeStruct((parts, rows, 3 * width), low),
            jax.ShapeDtypeStruct((parts, rows, width), low),
            jax.ShapeDtypeStruct((parts, rows, hidden), low),
            jax.ShapeDtypeStruct((parts, rows, hidden), low),
        ],
        in_specs=[
            whole((rows, D)),
            whole(gains.shape),
            pl.BlockSpec((1,) + block, lambda step: (base + early(step), 0, 0)),
            pl.BlockSpec((1,) + block, lambda step: (base + parts + late(step), 0, 0)),
            pl.BlockSpec((1,) + block, lambda step: (base + 2 * parts + late(step), 0, 0)),
            pl.BlockSpec((1, 1, 3 * width), lambda step: (early(step), 0, 0)),
            pl.BlockSpec((1, 1, hidden), lambda step: (late(step), 0, 0)),
        ],
        out_specs=[
            whole((rows, D)),
            whole((rows, D)),
            pl.BlockSpec((1, rows, 3 * width), lambda step: (early(step), 0, 0)),
            pl.BlockSpec((1, rows, width), lambda step: (early(step), 0, 0)),
            pl.BlockSpec((1, rows, hidden), lambda step: (late(step), 0, 0)),
            pl.BlockSpec((1, rows, hidden), lambda step: (late(step), 0, 0)),
        ],
        scratch_shapes=[pltpu.VMEM((rows, D), low)],
        compiler_params=pltpu.CompilerParams(vmem_limit_bytes=48 << 20),
    )(x, gains, weights, weights, weights, split_rows, hidden_rows)


def backward_kernel(
    images, parts, grad_ref, x_ref, mid_ref, gain_ref, attn_ref, up_ref, down_ref,
    qkv_ref, mixed_ref, act_ref, slope_ref,
    out_ref, attn_grad_ref, mlp_grad_ref, shared_ref, split_ref, hidden_ref,
    total, low_grad, turned_grad, turned_in,
):
    step = pl.program_id(0)
    low = jnp.bfloat16
    width = mixed_ref.shape[-1]
    heads = width // HEAD_DIM

    def row_sum(values):
        return jnp.sum(values, axis=0, keepdims=True)

    @pl.when(step == 0)
    def _():
        grad = grad_ref[...]
        shared_ref[5:6] = row_sum(grad)
        low_grad[...] = grad.astype(low)
        turned_grad[...] = grad.T.astype(low)
        unit, _ = normal_form(mid_ref[...])
        turned_in[...] = (unit * gain_ref[3:4] + gain_ref[4:5]).T.astype(low)
        total[...] = jnp.zeros_like(total)

    @pl.when(step < parts)
    def _():
        act_grad = dot_nn(low_grad[...], down_ref[0])
        mlp_grad_ref[1, 0] = dot_nn(turned_grad[...], act_ref[0]).astype(low)
        pre_grad = act_grad * slope_ref[0].astype(jnp.float32)
        hidden_ref[0] = row_sum(pre_grad)
        pre_low = pre_grad.astype(low)
        mlp_grad_ref[0, 0] = dot_nn(turned_in[...], pre_low).astype(low)
        total[...] += dot_nt(pre_low, up_ref[0])

    @pl.when(step == parts)
    def _():
        unit, inverse = normal_form(mid_ref[...])
        back = total[...]
        shared_ref[3:4] = row_sum(back * unit)
        shared_ref[4:5] = row_sum(back)
        grad = grad_ref[...] + norm_back(back, unit, inverse, gain_ref[3:4])
        out_ref[...] = grad
        shared_ref[2:3] = row_sum(grad)
        low_grad[...] = grad.astype(low)
        turned_grad[...] = grad.T.astype(low)
        unit, _ = normal_form(x_ref[...])
        turned_in[...] = (unit * gain_ref[0:1] + gain_ref[1:2]).T.astype(low)
        total[...] = jnp.zeros_like(total)

    @pl.when(step >= parts)
    def _():
        weights = attn_ref[0]
        qkv = qkv_ref[0]
        mixed_grad = dot_nn(low_grad[...], weights[:, 3 * width :]).astype(low)
        pieces = [[None] * heads for _ in range(3)]
        for head in range(heads):
            rows = [[], [], []]
            for image in range(images):
                at = slice(image * PAD_ROWS, (image + 1) * PAD_ROWS)
                query, key, value = (
                    qkv[at, kind * width + head * HEAD_DIM : kind * width + (head + 1) * HEAD_DIM]
                    for kind in range(3)
                )
                out_grad = mixed_grad[at, head * HEAD_DIM : (head + 1) * HEAD_DIM]
                probs = head_probs(query, key)
                prob_grad = dot_nt(out_grad, value)
                inner = jnp.sum(probs * prob_grad, axis=-1, keepdims=True)
                score_grad = (probs * (prob_grad - inner) * HEAD_DIM ** (-0.5)).astype(low)
                rows[0].append(dot_nn(score_grad, key))
                rows[1].append(dot_tn(score_grad, query))
                rows[2].append(dot_tn(probs.astype(low), out_grad))
            for kind in range(3):
                pieces[kind][head] = jnp.concatenate(rows[kind], axis=0)
        qkv_grad = jnp.concatenate(pieces[0] + pieces[1] + pieces[2], axis=1)
        split_ref[0] = row_sum(qkv_grad)
        qkv_low = qkv_grad.astype(low)
        attn_grad_ref[0, :, : 3 * width] = dot_nn(turned_in[...], qkv_low).astype(low)
        attn_grad_ref[0, :, 3 * width :] = dot_nn(turned_grad[...], mixed_ref[0]).astype(low)
        total[...] += dot_nt(qkv_low, weights[:, : 3 * width])

    @pl.when(step == 2 * parts - 1)
    def _():
        unit, inverse = normal_form(x_ref[...])
        back = total[...]
        shared_ref[0:1] = row_sum(back * unit)
        shared_ref[1:2] = row_sum(back)
        out_ref[...] += norm_back(back, unit, inverse, gain_ref[0:1])


def backward_layer(layer_idx, images, grad, x, mid, gains, weights, qkv, mixed, act, slope):
    rows = x.shape[0]
    parts = act.shape[0]
    base = layer_idx * 3 * parts
    width, hidden = mixed.shape[-1], act.shape[-1]
    block = weights.shape[1:]
    early = lambda step: jnp.minimum(step, parts - 1)
    late = lambda step: jnp.maximum(step - parts, 0)
    whole = lambda shape: pl.BlockSpec(shape, lambda step: (0,) * len(shape))
    low = jnp.bfloat16
    return pl.pallas_call(
        partial(backward_kernel, images, parts),
        grid=(2 * parts,),
        out_shape=[
            jax.ShapeDtypeStruct((rows, D), jnp.float32),
            jax.ShapeDtypeStruct((parts,) + block, low),
            jax.ShapeDtypeStruct((2, parts) + block, low),
            jax.ShapeDtypeStruct((6, D), jnp.float32),
            jax.ShapeDtypeStruct((parts, 1, 3 * width), jnp.float32),
            jax.ShapeDtypeStruct((parts, 1, hidden), jnp.float32),
        ],
        in_specs=[
            whole((rows, D)),
            whole((rows, D)),
            whole((rows, D)),
            whole(gains.shape),
            pl.BlockSpec((1,) + block, lambda step: (base + late(step), 0, 0)),
            pl.BlockSpec((1,) + block, lambda step: (base + parts + early(step), 0, 0)),
            pl.BlockSpec((1,) + block, lambda step: (base + 2 * parts + early(step), 0, 0)),
            pl.BlockSpec((1, rows, 3 * width), lambda step: (late(step), 0, 0)),
            pl.BlockSpec((1, rows, width), lambda step: (late(step), 0, 0)),
            pl.BlockSpec((1, rows, hidden), lambda step: (early(step), 0, 0)),
            pl.BlockSpec((1, rows, hidden), lambda step: (early(step), 0, 0)),
        ],
        out_specs=[
            whole((rows, D)),
            pl.BlockSpec((1,) + block, lambda step: (late(step), 0, 0)),
            pl.BlockSpec((2, 1) + block, lambda step: (0, early(step), 0, 0)),
            whole((6, D)),
            pl.BlockSpec((1, 1, 3 * width), lambda step: (late(step), 0, 0)),
            pl.BlockSpec((1, 1, hidden), lambda step: (early(step), 0, 0)),
        ],
        scratch_shapes=[
            pltpu.VMEM((rows, D), jnp.float32),
            pltpu.VMEM((rows, D), low),
            pltpu.VMEM((D, rows), low),
            pltpu.VMEM((D, rows), low),
        ],
        compiler_params=pltpu.CompilerParams(vmem_limit_bytes=56 << 20),
    )(grad, x, mid, gains, weights, weights, weights, qkv, mixed, act, slope)


MESH_SHAPE = (8, 4)
ROW_HALVES = 2
SMALL_WIDTH = 1024
LAYER_BLOCKS = 3


def hand_made():
    return (lax.axis_size("dp"), lax.axis_size("tensor")) == MESH_SHAPE


def device_rows_first(values):
    return values.transpose((0, 3, 4, 5, 1, 2) + tuple(range(6, values.ndim)))


def device_rows_last(values):
    return values.transpose((0, 4, 5, 1, 2, 3) + tuple(range(6, values.ndim)))


def gather_all(blocks, small, vectors):
    parts, depth = lax.axis_size("tensor"), lax.axis_size("dp")
    count, rows, columns = blocks.shape
    if hand_made():
        groups = (
            (((1, (0,), (), 0), (2, (), (), 1)),)
            + tuple(
                tuple((0, (at,), (half,), half) for half in range(ROW_HALVES))
                for at in range(count)
            )
            + (((1, (1,), (), 1),),)
        )
        halves = blocks.reshape(count, ROW_HALVES, rows // ROW_HALVES, columns)
        padded = jnp.pad(vectors, (0, -vectors.size % 1024)).reshape(-1, 128)
        wide, thin, lists = spread([halves, small, padded], groups, 1)
        thin = device_rows_first(thin)
        lists = lists[:, :, 0, 0, 0].reshape(parts, -1)[:, : vectors.size]
    else:
        both = ("dp", "tensor")
        wide = lax.all_gather(blocks, both, axis=0, tiled=False)
        wide = wide.reshape(depth, parts, count, rows, columns).transpose(2, 1, 0, 3, 4)
        thin = lax.all_gather(small, both, axis=1, tiled=True)
        lists = lax.all_gather(vectors, "tensor", axis=0, tiled=False)
    return (
        wide.reshape(count * parts, depth * rows, columns),
        thin.reshape(small.shape[0], -1, small.shape[-1]),
        lists,
    )


def sum_layer(attn_part, mlp_part):
    parts, depth = lax.axis_size("tensor"), lax.axis_size("dp")
    rows, columns = attn_part.shape[1] // depth, attn_part.shape[2]
    if hand_made():
        form = (2,) * len(DIMS) + (ROW_HALVES, rows // ROW_HALVES, columns)
        groups = tuple(
            tuple((1, (at,), (half,), half) for half in range(ROW_HALVES)) for at in range(2)
        ) + (tuple((0, (), (half,), half) for half in range(ROW_HALVES)),)
        attn_sum, mlp_sum = collect(
            [attn_part.reshape(form), mlp_part.reshape((2,) + form)], groups, 2
        )
    else:
        whole = jnp.concatenate([attn_part[None], mlp_part]).reshape(
            LAYER_BLOCKS, parts, depth, rows, columns
        )
        whole = whole.transpose(2, 1, 0, 3, 4).reshape(-1, LAYER_BLOCKS, rows, columns)
        total = lax.psum_scatter(
            whole, ("dp", "tensor"), scatter_dimension=0, tiled=False
        ).astype(jnp.float32)
        attn_sum, mlp_sum = total[0], total[1:]
    return attn_sum.reshape(rows, columns), mlp_sum.reshape(2, rows, columns)


def sum_small(small):
    devices = lax.axis_size("dp") * lax.axis_size("tensor")
    rows = small.shape[1] // devices
    if hand_made():
        form = device_rows_last(small.reshape((2,) + (2,) * len(DIMS) + (rows, SMALL_WIDTH)))
        groups = (tuple((0, (at,), (), at) for at in range(2)),)
        return collect([form], groups, 3)[0]
    blocks = small.reshape(2, devices, rows, -1).transpose(1, 0, 2, 3)
    return lax.psum_scatter(
        blocks, ("dp", "tensor"), scatter_dimension=0, tiled=False
    ).astype(jnp.float32)


def finish_step(weight, update, update_sq, weight_sq, entries):
    clip_factor = jnp.maximum(1.0, jnp.sqrt(update_sq / entries) / clip_level)
    step_size = step_ratio * jnp.maximum(floor_scale, jnp.sqrt(weight_sq / entries))
    return weight - step_size * update / clip_factor


def shards(
    patches, labels, image_count,
    attn_weight, attn_rows, attn_cols,
    mlp_weight, mlp_rows, mlp_cols,
    patch_weight, patch_rows, patch_cols,
    embed_table, embed_rows, embed_cols,
    head_weight, head_rows, head_cols,
    split_vec, split_sq, hidden_bias, hidden_sq,
    shared_vec, shared_sq, head_bias, head_bias_sq,
):
    both = ("dp", "tensor")
    low = jnp.bfloat16
    tensor_width = lax.axis_size("tensor")
    dp_width = lax.axis_size("dp")
    tensor_rank = lax.axis_index("tensor")
    shard_rank = lax.axis_index("dp")
    images = patches.shape[0]
    own_rows = attn_weight.shape[1]
    attn_width = attn_weight.shape[3]
    mlp_width = mlp_weight.shape[3]
    slot_index = tensor_rank * images + jnp.arange(images)
    image_total = jnp.sum(image_count).astype(jnp.float32)
    image_weight = (
        jnp.where(slot_index < image_count[shard_rank], 1.0, 0.0).astype(jnp.float32) / image_total
    )

    blocks = jnp.concatenate(
        [attn_weight.reshape(LAYERS, 1, own_rows, 4 * attn_width), mlp_weight], axis=1
    ).astype(low)
    widen = lambda values: jnp.pad(
        values, ((0, 0), (0, SMALL_WIDTH - values.shape[1]))
    )
    small = jnp.stack(
        [widen(jnp.concatenate([patch_weight, embed_table], axis=1)), widen(head_weight)]
    ).astype(low)
    weights, small_full, vectors = gather_all(
        blocks.reshape(LAYERS * LAYER_BLOCKS, own_rows, mlp_width),
        small,
        flatten_all([split_vec, hidden_bias]),
    )
    patch_full, table_full = small_full[0, :, :D], small_full[0, :, D : D + EXTRA]
    head_full = small_full[1, :, :CLASSES]
    split_rows = vectors[:, : split_vec.size].reshape(tensor_width, LAYERS, 2, attn_width)
    split_rows = jnp.stack(
        [split_rows[:, :, 0], jnp.zeros_like(split_rows[:, :, 0]), split_rows[:, :, 1]], axis=2
    ).reshape(tensor_width, LAYERS, 1, 3 * attn_width)
    hidden_rows = vectors[:, split_vec.size :].reshape(tensor_width, LAYERS, 1, mlp_width)

    table_rows = table_full.astype(jnp.float32).T
    pixel_rows = patches.reshape(images * (TOK_IMG - 1), PATCH)
    embedded = jnp.dot(pixel_rows, patch_full, preferred_element_type=jnp.float32).reshape(
        images, TOK_IMG - 1, D
    )
    embedded = embedded + table_rows[1:TOK_IMG] + table_rows[TOK_IMG]
    residual = jnp.concatenate(
        [
            jnp.broadcast_to(table_rows[0], (images, 1, D)),
            embedded,
            jnp.zeros((images, PAD_ROWS - TOK_IMG, D), jnp.float32),
        ],
        axis=1,
    ).reshape(images * PAD_ROWS, D)

    saved = []
    for layer_idx in range(LAYERS):
        gains = shared_vec[6 * layer_idx : 6 * layer_idx + 6]
        layer_input = residual
        residual, mid, qkv, mixed, act, slope = forward_layer(
            layer_idx, images, residual, gains, weights,
            split_rows[:, layer_idx], hidden_rows[:, layer_idx],
        )
        saved.append((layer_input, mid, gains, qkv, mixed, act, slope))
    cls_rows = residual.reshape(images, PAD_ROWS, D)[:, 0]
    feature, final_back = jax.vjp(
        layer_norm, cls_rows, shared_vec[6 * LAYERS], shared_vec[6 * LAYERS + 1]
    )
    feature_low = feature.astype(low)
    logits = jnp.dot(feature_low, head_full, preferred_element_type=jnp.float32) + head_bias
    log_norm = jax.nn.logsumexp(logits, axis=-1, keepdims=True)
    onehot = jnp.where(labels[:, None] == jnp.arange(CLASSES)[None, :], 1.0, 0.0).astype(
        jnp.float32
    )
    target = (1.0 - smoothing) * onehot + smoothing / CLASSES
    loss_part = jnp.sum((log_norm[:, 0] - jnp.sum(target * logits, axis=-1)) * image_weight)
    grad_logits = (jnp.exp(logits - log_norm) - target) * image_weight[:, None]
    grad_head_bias = jnp.sum(grad_logits, axis=0)
    logits_low = grad_logits.astype(low)
    grad_head = outer_sum(feature_low, logits_low)
    grad_feature = times_transposed(logits_low, head_full)
    grad_cls, grad_final_gain, grad_final_shift = final_back(grad_feature)
    grad_rows = jnp.concatenate(
        [grad_cls[:, None], jnp.zeros((images, PAD_ROWS - 1, D), jnp.float32)], axis=1
    ).reshape(images * PAD_ROWS, D)
    shared_list = [None] * LAYERS
    split_list = [None] * LAYERS
    hidden_list = [None] * LAYERS
    attn_list = [None] * LAYERS
    mlp_list = [None] * LAYERS
    for layer_idx in reversed(range(LAYERS)):
        layer_input, mid, gains, qkv, mixed, act, slope = saved[layer_idx]
        grad_rows, attn_part, mlp_part, shared_list[layer_idx], split_part, hidden_part = (
            backward_layer(
                layer_idx, images, grad_rows, layer_input, mid, gains, weights,
                qkv, mixed, act, slope,
            )
        )
        split_part = split_part.reshape(tensor_width, 3, attn_width)
        split_list[layer_idx] = jnp.stack([split_part[:, 0], split_part[:, 2]], axis=1)
        hidden_list[layer_idx] = hidden_part.reshape(tensor_width, mlp_width)
        attn_sum, mlp_list[layer_idx] = sum_layer(attn_part, mlp_part)
        attn_list[layer_idx] = attn_sum.reshape(own_rows, 4, attn_width)
    grad_image = grad_rows.reshape(images, PAD_ROWS, D)
    grad_first = jnp.sum(grad_image[:, 0], axis=0)
    grad_position = jnp.sum(grad_image[:, 1:TOK_IMG], axis=0)
    grad_patch_bias = jnp.sum(grad_position, axis=0)
    embed_low = grad_image[:, 1:TOK_IMG].astype(low).reshape(images * (TOK_IMG - 1), D)
    grad_patch = outer_sum(pixel_rows, embed_low)
    grad_table = jnp.concatenate([grad_first[None], grad_position, grad_patch_bias[None]], axis=0).T
    small_sum = sum_small(
        jnp.stack(
            [widen(jnp.concatenate([grad_patch, grad_table], axis=1)), widen(grad_head)]
        ).astype(low)
    )
    patch_grad, table_grad = small_sum[0, :, :D], small_sum[0, :, D : D + EXTRA]
    head_grad = small_sum[1, :, :CLASSES]
    attn_grad = jnp.stack(attn_list)
    mlp_grad = jnp.stack(mlp_list)
    shared_grad = jnp.concatenate(
        shared_list + [jnp.stack([grad_final_gain, grad_final_shift])], axis=0
    )
    attn_sq = attn_grad * attn_grad
    mlp_sq = mlp_grad * mlp_grad
    patch_sq = patch_grad * patch_grad
    table_sq = table_grad * table_grad
    head_sq = head_grad * head_grad

    split_sums, hidden_sums, shared_full, head_bias_full, loss_total = summed_over(
        both,
        [jnp.stack(split_list, 1), jnp.stack(hidden_list, 1), shared_grad, grad_head_bias, loss_part],
    )
    split_total = lax.dynamic_index_in_dim(split_sums, tensor_rank, 0, keepdims=False)
    hidden_total = lax.dynamic_index_in_dim(hidden_sums, tensor_rank, 0, keepdims=False)
    attn_row_full, mlp_row_full = summed_over(
        "tensor", [jnp.sum(attn_sq, axis=3).transpose(0, 2, 1), jnp.sum(mlp_sq, axis=3)]
    )
    attn_col_full, mlp_col_full = summed_over("dp", [jnp.sum(attn_sq, axis=1), jnp.sum(mlp_sq, axis=2)])
    attn_row_new = decay_rate * attn_rows + (1.0 - decay_rate) * (attn_row_full / D + tiny_sq)
    mlp_row_new = decay_rate * mlp_rows + (1.0 - decay_rate) * (mlp_row_full / FF + tiny_sq)
    patch_row_new = decay_rate * patch_rows + (1.0 - decay_rate) * (
        jnp.sum(patch_sq, axis=1) / D + tiny_sq
    )
    table_row_new = decay_rate * embed_rows + (1.0 - decay_rate) * (
        jnp.sum(table_sq, axis=1) / EXTRA + tiny_sq
    )
    head_row_new = decay_rate * head_rows + (1.0 - decay_rate) * (
        jnp.sum(head_sq, axis=1) / CLASSES + tiny_sq
    )
    own_share = 1.0 / tensor_width
    (
        patch_col_full, table_col_full, head_col_full, whole_row_sum,
        attn_old_sum, mlp_old_sum, attn_total, mlp_total, weight_sq_parts,
    ) = summed_over(
        both,
        [
            jnp.sum(patch_sq, axis=0),
            jnp.sum(table_sq, axis=0),
            jnp.sum(head_sq, axis=0),
            jnp.stack([jnp.sum(patch_row_new), jnp.sum(table_row_new), jnp.sum(head_row_new)]),
            jnp.sum(attn_rows, axis=-1) * own_share,
            jnp.sum(mlp_rows, axis=-1) * own_share,
            jnp.sum(attn_sq, axis=(1, 3)),
            jnp.sum(mlp_sq, axis=(2, 3)),
            flatten_all(
                [
                    jnp.sum(attn_weight * attn_weight, axis=(1, 3)),
                    jnp.sum(mlp_weight * mlp_weight, axis=(2, 3)),
                    jnp.sum(patch_weight * patch_weight),
                    jnp.sum(embed_table * embed_table),
                    jnp.sum(head_weight * head_weight),
                ]
            ),
        ],
    )
    weight_sq = split_all(weight_sq_parts, [(LAYERS, 4), (LAYERS, 2), (), (), ()])
    attn_row_mean = (
        decay_rate * attn_old_sum + (1.0 - decay_rate) * (attn_total / D + D * tiny_sq)
    ) / D
    mlp_row_mean = (
        decay_rate * mlp_old_sum + (1.0 - decay_rate) * (mlp_total / FF + D * tiny_sq)
    ) / D
    whole_row_mean = whole_row_sum / jnp.array([PATCH, D, D], jnp.float32)
    attn_col_new = decay_rate * attn_cols + (1.0 - decay_rate) * (attn_col_full / D + tiny_sq)
    mlp_col_new = decay_rate * mlp_cols + (1.0 - decay_rate) * (mlp_col_full / D + tiny_sq)
    patch_col_new = decay_rate * patch_cols + (1.0 - decay_rate) * (
        patch_col_full / PATCH + tiny_sq
    )
    table_col_new = decay_rate * embed_cols + (1.0 - decay_rate) * (table_col_full / D + tiny_sq)
    head_col_new = decay_rate * head_cols + (1.0 - decay_rate) * (head_col_full / D + tiny_sq)
    attn_update = attn_grad * lax.rsqrt(
        attn_row_new.transpose(0, 2, 1)[:, :, :, None]
        * attn_col_new[:, None]
        / attn_row_mean[:, None, :, None]
    )
    mlp_update = mlp_grad * lax.rsqrt(
        mlp_row_new[:, :, :, None] * mlp_col_new[:, :, None, :] / mlp_row_mean[:, :, None, None]
    )
    patch_update = patch_grad * lax.rsqrt(
        patch_row_new[:, None] * patch_col_new[None, :] / whole_row_mean[0]
    )
    table_update = table_grad * lax.rsqrt(
        table_row_new[:, None] * table_col_new[None, :] / whole_row_mean[1]
    )
    head_update = head_grad * lax.rsqrt(
        head_row_new[:, None] * head_col_new[None, :] / whole_row_mean[2]
    )
    split_sq_new = decay_rate * split_sq + (1.0 - decay_rate) * (
        split_total * split_total + tiny_sq
    )
    split_update = split_total * lax.rsqrt(split_sq_new)
    hidden_sq_new = decay_rate * hidden_sq + (1.0 - decay_rate) * (
        hidden_total * hidden_total + tiny_sq
    )
    hidden_update = hidden_total * lax.rsqrt(hidden_sq_new)
    shared_sq_new = decay_rate * shared_sq + (1.0 - decay_rate) * (
        shared_full * shared_full + tiny_sq
    )
    shared_update = shared_full * lax.rsqrt(shared_sq_new)
    head_bias_sq_new = decay_rate * head_bias_sq + (1.0 - decay_rate) * (
        head_bias_full * head_bias_full + tiny_sq
    )
    head_bias_update = head_bias_full * lax.rsqrt(head_bias_sq_new)
    dp_share = 1.0 / dp_width
    attn_u2, mlp_u2, patch_u2, table_u2, head_u2, split_u2, hidden_u2, split_w2, hidden_w2 = (
        summed_over(
            both,
            [
                jnp.sum(attn_update * attn_update, axis=(1, 3)),
                jnp.sum(mlp_update * mlp_update, axis=(2, 3)),
                jnp.sum(patch_update * patch_update),
                jnp.sum(table_update * table_update),
                jnp.sum(head_update * head_update),
                jnp.sum(split_update * split_update, axis=-1) * dp_share,
                jnp.sum(hidden_update * hidden_update, axis=-1) * dp_share,
                jnp.sum(split_vec * split_vec, axis=-1) * dp_share,
                jnp.sum(hidden_bias * hidden_bias, axis=-1) * dp_share,
            ],
        )
    )
    vector_sq = [split_w2, hidden_w2]
    attn_new = finish_step(
        attn_weight, attn_update, attn_u2[:, None, :, None], weight_sq[0][:, None, :, None], D * D
    )
    mlp_new = finish_step(
        mlp_weight, mlp_update, mlp_u2[:, :, None, None], weight_sq[1][:, :, None, None], D * FF
    )
    patch_new = finish_step(patch_weight, patch_update, patch_u2, weight_sq[2], PATCH * D)
    embed_new = finish_step(embed_table, table_update, table_u2, weight_sq[3], D * EXTRA)
    head_new = finish_step(head_weight, head_update, head_u2, weight_sq[4], D * CLASSES)
    split_new = finish_step(
        split_vec, split_update, split_u2[:, :, None], vector_sq[0][:, :, None], D
    )
    hidden_new = finish_step(
        hidden_bias, hidden_update, hidden_u2[:, None], vector_sq[1][:, None], FF
    )
    shared_new = finish_step(
        shared_vec,
        shared_update,
        jnp.sum(shared_update * shared_update, axis=-1, keepdims=True),
        jnp.sum(shared_vec * shared_vec, axis=-1, keepdims=True),
        D,
    )
    head_bias_new = finish_step(
        head_bias,
        head_bias_update,
        jnp.sum(head_bias_update * head_bias_update),
        jnp.sum(head_bias * head_bias),
        CLASSES,
    )
    return (
        loss_total,
        attn_new,
        attn_row_new,
        attn_col_new,
        mlp_new,
        mlp_row_new,
        mlp_col_new,
        patch_new,
        patch_row_new,
        patch_col_new,
        embed_new,
        table_row_new,
        table_col_new,
        head_new,
        head_row_new,
        head_col_new,
        split_new,
        split_sq_new,
        hidden_new,
        hidden_sq_new,
        shared_new,
        shared_sq_new,
        head_bias_new,
        head_bias_sq_new,
    )


def solution(mesh):
    in_specs = (
        P(("dp", "tensor"), None, None),
        P(("dp", "tensor")),
        P(),
        P(None, "dp", None, "tensor"),
        P(None, None, "dp"),
        P(None, None, "tensor"),
        P(None, None, "dp", "tensor"),
        P(None, None, "dp"),
        P(None, None, "tensor"),
        P(("dp", "tensor"), None),
        P(("dp", "tensor")),
        P(),
        P(("dp", "tensor"), None),
        P(("dp", "tensor")),
        P(),
        P(("dp", "tensor"), None),
        P(("dp", "tensor")),
        P(),
        P(None, None, "tensor"),
        P(None, None, "tensor"),
        P(None, "tensor"),
        P(None, "tensor"),
        P(),
        P(),
        P(),
        P(),
    )
    out_specs = (
        P(),
        P(None, "dp", None, "tensor"),
        P(None, None, "dp"),
        P(None, None, "tensor"),
        P(None, None, "dp", "tensor"),
        P(None, None, "dp"),
        P(None, None, "tensor"),
        P(("dp", "tensor"), None),
        P(("dp", "tensor")),
        P(),
        P(("dp", "tensor"), None),
        P(("dp", "tensor")),
        P(),
        P(("dp", "tensor"), None),
        P(("dp", "tensor")),
        P(),
        P(None, None, "tensor"),
        P(None, None, "tensor"),
        P(None, "tensor"),
        P(None, "tensor"),
        P(),
        P(),
        P(),
        P(),
    )
    return jax.shard_map(shards, mesh=mesh, in_specs=in_specs, out_specs=out_specs, check_vma=False)
```

```python
from functools import partial
import math

import jax
import jax.numpy as jnp
from jax import lax
from jax.experimental import pallas as pl
from jax.experimental.pallas import tpu as pltpu
from jax.sharding import PartitionSpec as P

D = 768
HEAD_DIM = 64
FF = 3072
PATCH = 768
CLASSES = 1000
TOK_IMG = 197
LAYERS = 3
SEQ = 200
EXTRA = 198


decay_rate = 0.5
tiny_sq = 1e-30
floor_scale = 0.001
step_ratio = 1.0
clip_level = 0.1
smoothing = 0.1
norm_eps = 1e-06


def layer_norm(values, gain_vec, shift_vec):
    centred = values - jnp.mean(values, axis=-1, keepdims=True)
    spread = jnp.mean(centred * centred, axis=-1, keepdims=True)
    return centred * lax.rsqrt(spread + norm_eps) * gain_vec + shift_vec


def outer_sum(left_rows, right_rows):
    return lax.dot_general(
        left_rows, right_rows, (((0,), (0,)), ((), ())), preferred_element_type=jnp.float32
    )


def times_transposed(left_rows, right_matrix):
    return lax.dot_general(
        left_rows, right_matrix, (((1,), (1,)), ((), ())), preferred_element_type=jnp.float32
    )


def flatten_all(arrays):
    return jnp.concatenate([jnp.ravel(member) for member in arrays])


def split_all(flat, shapes):
    outputs = []
    offset = 0
    for form_shape in shapes:
        length = math.prod(form_shape)
        outputs.append(flat[offset : offset + length].reshape(form_shape))
        offset = offset + length
    return outputs


def summed_over(axes, arrays):
    return split_all(
        lax.psum(flatten_all(arrays), axes), [member.shape for member in arrays]
    )


MESH = pl.DeviceIdType.MESH
DIMS = ("y", "c", "zb", "za", "x")
OUT_ORDERS = (("zb", "x", "za", "y", "c"), ("zb", "y", "za", "x", "c"))
IN_ORDERS = tuple(order[::-1] for order in OUT_ORDERS)


def place_of_device():
    dp, tensor = lax.axis_index("dp"), lax.axis_index("tensor")
    return {
        "x": lax.rem(dp, 2),
        "za": lax.rem(dp // 2, 2),
        "zb": dp // 4,
        "y": tensor // 2,
        "c": lax.rem(tensor, 2),
    }


def partner_of(place, dim):
    moved = dict(place)
    moved[dim] = 1 - place[dim]
    return (
        moved["zb"] * 4 + moved["za"] * 2 + moved["x"],
        moved["y"] * 2 + moved["c"],
    )


def meet_partners(place):
    barrier = pltpu.get_barrier_semaphore()
    for dim in DIMS:
        pl.semaphore_signal(
            barrier, inc=1, device_id=partner_of(place, dim), device_id_type=MESH
        )
    pl.semaphore_wait(barrier, len(DIMS))


def spread_kernel(groups, *refs):
    arrays = len({flow[0] for group in groups for flow in group})
    sources, targets = refs[:arrays], refs[arrays : 2 * arrays]
    send_sem, recv_sem, own_sem = refs[2 * arrays :]
    place = place_of_device()
    flows = [flow for group in groups for flow in group]
    number = {flow: position for position, flow in enumerate(flows)}

    def own_copy(flow):
        array, lead, tail, _ = flow
        slot = lead + tuple(place[dim] for dim in DIMS) + tail
        return pltpu.make_async_copy(
            sources[array].at[lead + tail], targets[array].at[slot], own_sem.at[number[flow]]
        )

    def stage_copy(flow, stage):
        array, lead, tail, order = flow
        dims = OUT_ORDERS[order]
        done = dims[:stage]
        slot = lead + tuple(slice(None) if dim in done else place[dim] for dim in DIMS) + tail
        source = sources[array].at[lead + tail] if stage == 0 else targets[array].at[slot]
        return pltpu.make_async_remote_copy(
            src_ref=source,
            dst_ref=targets[array].at[slot],
            send_sem=send_sem.at[number[flow], stage],
            recv_sem=recv_sem.at[number[flow], stage],
            device_id=partner_of(place, dims[stage]),
            device_id_type=MESH,
        )

    meet_partners(place)
    stages = len(DIMS)
    for tick in range(len(groups) + stages):
        for stage in reversed(range(stages + 1)):
            if not 0 <= tick - stage < len(groups):
                continue
            for flow in groups[tick - stage]:
                if stage == 1:
                    own_copy(flow).wait()
                if stage > 0:
                    stage_copy(flow, stage - 1).wait_recv()
                if stage == 0:
                    own_copy(flow).start()
                if stage < stages:
                    stage_copy(flow, stage).start()
    for flow in flows:
        for stage in range(stages):
            stage_copy(flow, stage).wait_send()


def spread(arrays, groups, collective_id):
    count = sum(len(group) for group in groups)
    leads = {flow[0]: len(flow[1]) for group in groups for flow in group}
    shapes = [
        member.shape[: leads[position]] + (2,) * len(DIMS) + member.shape[leads[position] :]
        for position, member in enumerate(arrays)
    ]
    return pl.pallas_call(
        partial(spread_kernel, groups),
        out_shape=[
            jax.ShapeDtypeStruct(shape, member.dtype) for shape, member in zip(shapes, arrays)
        ],
        in_specs=[pl.BlockSpec(memory_space=pltpu.VMEM)] * len(arrays),
        out_specs=[pl.BlockSpec(memory_space=pl.ANY)] * len(arrays),
        scratch_shapes=[
            pltpu.SemaphoreType.DMA((count, len(DIMS))),
            pltpu.SemaphoreType.DMA((count, len(DIMS))),
            pltpu.SemaphoreType.DMA((count,)),
        ],
        compiler_params=pltpu.CompilerParams(
            collective_id=collective_id, has_side_effects=True, vmem_limit_bytes=16 << 20
        ),
    )(*arrays)


def collect_kernel(groups, arrays, *refs):
    sources, targets = refs[:arrays], refs[arrays : 2 * arrays]
    held, landed = refs[2 * arrays], refs[2 * arrays + 1 : 2 * arrays + 6]
    send_sem, recv_sem, own_sem = refs[2 * arrays + 6 :]
    place = place_of_device()
    flows = [flow for group in groups for flow in group]
    number = {flow: position for position, flow in enumerate(flows)}
    kept = ("y", "zb", "za", "x")

    def core_slot(flow, core):
        _, lead, tail, _ = flow
        return lead + tuple(core if dim == "c" else slice(None) for dim in DIMS) + tail

    def own_copy(flow):
        return pltpu.make_async_copy(
            sources[flow[0]].at[core_slot(flow, place["c"])],
            held.at[number[flow]],
            own_sem.at[number[flow]],
        )

    def held_slot(done, moved):
        slot = ()
        for dim in kept:
            if dim == moved:
                slot += (1 - place[dim],)
            elif dim in done:
                slot += (place[dim],)
            else:
                slot += (slice(None),)
        return slot

    def stage_copy(flow, stage):
        dims = IN_ORDERS[flow[3]]
        index = number[flow]
        if stage == 0:
            source = sources[flow[0]].at[core_slot(flow, 1 - place["c"])]
        else:
            source = held.at[(index,) + held_slot(dims[:stage], dims[stage])]
        return pltpu.make_async_remote_copy(
            src_ref=source,
            dst_ref=landed[stage].at[index],
            send_sem=send_sem.at[index, stage],
            recv_sem=recv_sem.at[index, stage],
            device_id=partner_of(place, dims[stage]),
            device_id_type=MESH,
        )

    def add_landed(flow, stage):
        array, lead, tail, order = flow
        dims = IN_ORDERS[order]
        index = number[flow]
        free = [dim for dim in kept if dim not in dims[: stage + 1]]

        def add_block(step, carry):
            rest = step
            at = {}
            for dim in reversed(free):
                at[dim] = lax.rem(rest, 2)
                rest = rest // 2
            slot = (index,) + tuple(at[dim] if dim in free else place[dim] for dim in kept)
            landed_slot = (index,) + tuple(at[dim] for dim in free)
            total = held[slot].astype(jnp.float32) + landed[stage][landed_slot].astype(jnp.float32)
            if stage == len(DIMS) - 1:
                targets[array][lead + tail] = total
            else:
                held[slot] = total.astype(jnp.bfloat16)
            return carry

        if free:
            lax.fori_loop(0, 2 ** len(free), add_block, 0)
        else:
            add_block(0, 0)

    meet_partners(place)
    stages = len(DIMS)
    for tick in range(len(groups) + stages):
        for stage in reversed(range(stages + 1)):
            if not 0 <= tick - stage < len(groups):
                continue
            for flow in groups[tick - stage]:
                if stage == 0:
                    own_copy(flow).start()
                if stage == 1:
                    own_copy(flow).wait()
                if stage > 0:
                    stage_copy(flow, stage - 1).wait_recv()
                    add_landed(flow, stage - 1)
                if stage < stages:
                    stage_copy(flow, stage).start()
    for flow in flows:
        for stage in range(stages):
            stage_copy(flow, stage).wait_send()


def collect(arrays, groups, collective_id):
    leads = {flow[0]: len(flow[1]) for group in groups for flow in group}
    count = sum(len(group) for group in groups)
    block = arrays[0].shape[-2:]
    low = jnp.bfloat16
    return pl.pallas_call(
        partial(collect_kernel, groups, len(arrays)),
        out_shape=[
            jax.ShapeDtypeStruct(
                member.shape[: leads[position]] + member.shape[leads[position] + len(DIMS) :],
                jnp.float32,
            )
            for position, member in enumerate(arrays)
        ],
        in_specs=[pl.BlockSpec(memory_space=pl.ANY)] * len(arrays),
        out_specs=[pl.BlockSpec(memory_space=pltpu.VMEM)] * len(arrays),
        scratch_shapes=[
            pltpu.VMEM((count, 2, 2, 2, 2) + block, low),
            pltpu.VMEM((count, 2, 2, 2, 2) + block, low),
            pltpu.VMEM((count, 2, 2, 2) + block, low),
            pltpu.VMEM((count, 2, 2) + block, low),
            pltpu.VMEM((count, 2) + block, low),
            pltpu.VMEM((count,) + block, low),
            pltpu.SemaphoreType.DMA((count, len(DIMS))),
            pltpu.SemaphoreType.DMA((count, len(DIMS))),
            pltpu.SemaphoreType.DMA((count,)),
        ],
        compiler_params=pltpu.CompilerParams(
            collective_id=collective_id, has_side_effects=True, vmem_limit_bytes=48 << 20
        ),
    )(*arrays)


PAD_ROWS = 208
HALF_ROOT = 0.7071067811865476
DENSITY = 0.3989422804014327


def dot_nn(left, right):
    return lax.dot_general(left, right, (((1,), (0,)), ((), ())), preferred_element_type=jnp.float32)


def dot_nt(left, right):
    return lax.dot_general(left, right, (((1,), (1,)), ((), ())), preferred_element_type=jnp.float32)


def dot_tn(left, right):
    return lax.dot_general(left, right, (((0,), (0,)), ((), ())), preferred_element_type=jnp.float32)


def normal_form(values):
    centred = values - jnp.mean(values, axis=-1, keepdims=True)
    spread_sq = jnp.mean(centred * centred, axis=-1, keepdims=True)
    inverse = lax.rsqrt(spread_sq + norm_eps)
    return centred * inverse, inverse


def norm_back(grad, unit, inverse, gain):
    inner = grad * gain
    return inverse * (
        inner
        - jnp.mean(inner, axis=-1, keepdims=True)
        - unit * jnp.mean(inner * unit, axis=-1, keepdims=True)
    )


def head_probs(query, key):
    scores = dot_nt(query, key) * HEAD_DIM ** (-0.5)
    column = lax.broadcasted_iota(jnp.int32, scores.shape, 1)
    scores = jnp.where(column < TOK_IMG, scores, -1e30)
    powers = jnp.exp(scores - jnp.max(scores, axis=-1, keepdims=True))
    return powers / jnp.sum(powers, axis=-1, keepdims=True)


def forward_kernel(
    images, parts, x_ref, gain_ref, attn_ref, up_ref, down_ref, split_ref, hidden_ref,
    next_ref, mid_ref, qkv_ref, mixed_ref, act_ref, slope_ref, normed,
):
    step = pl.program_id(0)
    low = jnp.bfloat16
    width = mixed_ref.shape[-1]
    heads = width // HEAD_DIM

    @pl.when(step == 0)
    def _():
        unit, _ = normal_form(x_ref[...])
        normed[...] = (unit * gain_ref[0:1] + gain_ref[1:2]).astype(low)
        mid_ref[...] = x_ref[...] + gain_ref[2:3]

    @pl.when(step < parts)
    def _():
        weights = attn_ref[0]
        qkv = (dot_nn(normed[...], weights[:, : 3 * width]) + split_ref[0]).astype(low)
        qkv_ref[0] = qkv
        columns = []
        for head in range(heads):
            rows = []
            for image in range(images):
                at = slice(image * PAD_ROWS, (image + 1) * PAD_ROWS)
                query, key, value = (
                    qkv[at, kind * width + head * HEAD_DIM : kind * width + (head + 1) * HEAD_DIM]
                    for kind in range(3)
                )
                probs = head_probs(query, key).astype(low)
                rows.append(dot_nn(probs, value).astype(low))
            columns.append(jnp.concatenate(rows, axis=0))
        mixed = jnp.concatenate(columns, axis=1)
        mixed_ref[0] = mixed
        mid_ref[...] += dot_nt(mixed, weights[:, 3 * width :])

    @pl.when(step == parts)
    def _():
        unit, _ = normal_form(mid_ref[...])
        normed[...] = (unit * gain_ref[3:4] + gain_ref[4:5]).astype(low)
        next_ref[...] = mid_ref[...] + gain_ref[5:6]

    @pl.when(step >= parts)
    def _():
        pre = dot_nn(normed[...], up_ref[0]) + hidden_ref[0]
        share = 0.5 * (1.0 + lax.erf(pre * HALF_ROOT))
        act = (pre * share).astype(low)
        act_ref[0] = act
        slope_ref[0] = (share + pre * (DENSITY * jnp.exp(-0.5 * pre * pre))).astype(low)
        next_ref[...] += dot_nt(act, down_ref[0])


def forward_layer(layer_idx, images, x, gains, weights, split_rows, hidden_rows):
    rows = x.shape[0]
    parts = hidden_rows.shape[0]
    base = layer_idx * 3 * parts
    width, hidden = split_rows.shape[-1] // 3, hidden_rows.shape[-1]
    block = weights.shape[1:]
    early = lambda step: jnp.minimum(step, parts - 1)
    late = lambda step: jnp.maximum(step - parts, 0)
    whole = lambda shape: pl.BlockSpec(shape, lambda step: (0,) * len(shape))
    low = jnp.bfloat16
    return pl.pallas_call(
        partial(forward_kernel, images, parts),
        grid=(2 * parts,),
        out_shape=[
            jax.ShapeDtypeStruct((rows, D), jnp.float32),
            jax.ShapeDtypeStruct((rows, D), jnp.float32),
            jax.ShapeDtypeStruct((parts, rows, 3 * width), low),
            jax.ShapeDtypeStruct((parts, rows, width), low),
            jax.ShapeDtypeStruct((parts, rows, hidden), low),
            jax.ShapeDtypeStruct((parts, rows, hidden), low),
        ],
        in_specs=[
            whole((rows, D)),
            whole(gains.shape),
            pl.BlockSpec((1,) + block, lambda step: (base + early(step), 0, 0)),
            pl.BlockSpec((1,) + block, lambda step: (base + parts + late(step), 0, 0)),
            pl.BlockSpec((1,) + block, lambda step: (base + 2 * parts + late(step), 0, 0)),
            pl.BlockSpec((1, 1, 3 * width), lambda step: (early(step), 0, 0)),
            pl.BlockSpec((1, 1, hidden), lambda step: (late(step), 0, 0)),
        ],
        out_specs=[
            whole((rows, D)),
            whole((rows, D)),
            pl.BlockSpec((1, rows, 3 * width), lambda step: (early(step), 0, 0)),
            pl.BlockSpec((1, rows, width), lambda step: (early(step), 0, 0)),
            pl.BlockSpec((1, rows, hidden), lambda step: (late(step), 0, 0)),
            pl.BlockSpec((1, rows, hidden), lambda step: (late(step), 0, 0)),
        ],
        scratch_shapes=[pltpu.VMEM((rows, D), low)],
        compiler_params=pltpu.CompilerParams(vmem_limit_bytes=48 << 20),
    )(x, gains, weights, weights, weights, split_rows, hidden_rows)


def backward_kernel(
    images, parts, grad_ref, x_ref, mid_ref, gain_ref, attn_ref, up_ref, down_ref,
    qkv_ref, mixed_ref, act_ref, slope_ref,
    out_ref, attn_grad_ref, mlp_grad_ref, shared_ref, split_ref, hidden_ref,
    total, low_grad, turned_grad, turned_in,
):
    step = pl.program_id(0)
    low = jnp.bfloat16
    width = mixed_ref.shape[-1]
    heads = width // HEAD_DIM

    def row_sum(values):
        return jnp.sum(values, axis=0, keepdims=True)

    @pl.when(step == 0)
    def _():
        grad = grad_ref[...]
        shared_ref[5:6] = row_sum(grad)
        low_grad[...] = grad.astype(low)
        turned_grad[...] = grad.T.astype(low)
        unit, _ = normal_form(mid_ref[...])
        turned_in[...] = (unit * gain_ref[3:4] + gain_ref[4:5]).T.astype(low)
        total[...] = jnp.zeros_like(total)

    @pl.when(step < parts)
    def _():
        act_grad = dot_nn(low_grad[...], down_ref[0])
        mlp_grad_ref[1, 0] = dot_nn(turned_grad[...], act_ref[0]).astype(low)
        pre_grad = act_grad * slope_ref[0].astype(jnp.float32)
        hidden_ref[0] = row_sum(pre_grad)
        pre_low = pre_grad.astype(low)
        mlp_grad_ref[0, 0] = dot_nn(turned_in[...], pre_low).astype(low)
        total[...] += dot_nt(pre_low, up_ref[0])

    @pl.when(step == parts)
    def _():
        unit, inverse = normal_form(mid_ref[...])
        back = total[...]
        shared_ref[3:4] = row_sum(back * unit)
        shared_ref[4:5] = row_sum(back)
        grad = grad_ref[...] + norm_back(back, unit, inverse, gain_ref[3:4])
        out_ref[...] = grad
        shared_ref[2:3] = row_sum(grad)
        low_grad[...] = grad.astype(low)
        turned_grad[...] = grad.T.astype(low)
        unit, _ = normal_form(x_ref[...])
        turned_in[...] = (unit * gain_ref[0:1] + gain_ref[1:2]).T.astype(low)
        total[...] = jnp.zeros_like(total)

    @pl.when(step >= parts)
    def _():
        weights = attn_ref[0]
        qkv = qkv_ref[0]
        mixed_grad = dot_nn(low_grad[...], weights[:, 3 * width :]).astype(low)
        pieces = [[None] * heads for _ in range(3)]
        for head in range(heads):
            rows = [[], [], []]
            for image in range(images):
                at = slice(image * PAD_ROWS, (image + 1) * PAD_ROWS)
                query, key, value = (
                    qkv[at, kind * width + head * HEAD_DIM : kind * width + (head + 1) * HEAD_DIM]
                    for kind in range(3)
                )
                out_grad = mixed_grad[at, head * HEAD_DIM : (head + 1) * HEAD_DIM]
                probs = head_probs(query, key)
                prob_grad = dot_nt(out_grad, value)
                inner = jnp.sum(probs * prob_grad, axis=-1, keepdims=True)
                score_grad = (probs * (prob_grad - inner) * HEAD_DIM ** (-0.5)).astype(low)
                rows[0].append(dot_nn(score_grad, key))
                rows[1].append(dot_tn(score_grad, query))
                rows[2].append(dot_tn(probs.astype(low), out_grad))
            for kind in range(3):
                pieces[kind][head] = jnp.concatenate(rows[kind], axis=0)
        qkv_grad = jnp.concatenate(pieces[0] + pieces[1] + pieces[2], axis=1)
        split_ref[0] = row_sum(qkv_grad)
        qkv_low = qkv_grad.astype(low)
        attn_grad_ref[0, :, : 3 * width] = dot_nn(turned_in[...], qkv_low).astype(low)
        attn_grad_ref[0, :, 3 * width :] = dot_nn(turned_grad[...], mixed_ref[0]).astype(low)
        total[...] += dot_nt(qkv_low, weights[:, : 3 * width])

    @pl.when(step == 2 * parts - 1)
    def _():
        unit, inverse = normal_form(x_ref[...])
        back = total[...]
        shared_ref[0:1] = row_sum(back * unit)
        shared_ref[1:2] = row_sum(back)
        out_ref[...] += norm_back(back, unit, inverse, gain_ref[0:1])


def backward_layer(layer_idx, images, grad, x, mid, gains, weights, qkv, mixed, act, slope):
    rows = x.shape[0]
    parts = act.shape[0]
    base = layer_idx * 3 * parts
    width, hidden = mixed.shape[-1], act.shape[-1]
    block = weights.shape[1:]
    early = lambda step: jnp.minimum(step, parts - 1)
    late = lambda step: jnp.maximum(step - parts, 0)
    whole = lambda shape: pl.BlockSpec(shape, lambda step: (0,) * len(shape))
    low = jnp.bfloat16
    return pl.pallas_call(
        partial(backward_kernel, images, parts),
        grid=(2 * parts,),
        out_shape=[
            jax.ShapeDtypeStruct((rows, D), jnp.float32),
            jax.ShapeDtypeStruct((parts,) + block, low),
            jax.ShapeDtypeStruct((2, parts) + block, low),
            jax.ShapeDtypeStruct((6, D), jnp.float32),
            jax.ShapeDtypeStruct((parts, 1, 3 * width), jnp.float32),
            jax.ShapeDtypeStruct((parts, 1, hidden), jnp.float32),
        ],
        in_specs=[
            whole((rows, D)),
            whole((rows, D)),
            whole((rows, D)),
            whole(gains.shape),
            pl.BlockSpec((1,) + block, lambda step: (base + late(step), 0, 0)),
            pl.BlockSpec((1,) + block, lambda step: (base + parts + early(step), 0, 0)),
            pl.BlockSpec((1,) + block, lambda step: (base + 2 * parts + early(step), 0, 0)),
            pl.BlockSpec((1, rows, 3 * width), lambda step: (late(step), 0, 0)),
            pl.BlockSpec((1, rows, width), lambda step: (late(step), 0, 0)),
            pl.BlockSpec((1, rows, hidden), lambda step: (early(step), 0, 0)),
            pl.BlockSpec((1, rows, hidden), lambda step: (early(step), 0, 0)),
        ],
        out_specs=[
            whole((rows, D)),
            pl.BlockSpec((1,) + block, lambda step: (late(step), 0, 0)),
            pl.BlockSpec((2, 1) + block, lambda step: (0, early(step), 0, 0)),
            whole((6, D)),
            pl.BlockSpec((1, 1, 3 * width), lambda step: (late(step), 0, 0)),
            pl.BlockSpec((1, 1, hidden), lambda step: (early(step), 0, 0)),
        ],
        scratch_shapes=[
            pltpu.VMEM((rows, D), jnp.float32),
            pltpu.VMEM((rows, D), low),
            pltpu.VMEM((D, rows), low),
            pltpu.VMEM((D, rows), low),
        ],
        compiler_params=pltpu.CompilerParams(vmem_limit_bytes=56 << 20),
    )(grad, x, mid, gains, weights, weights, weights, qkv, mixed, act, slope)


MESH_SHAPE = (8, 4)
ROW_HALVES = 2
SMALL_WIDTH = 1024
LAYER_BLOCKS = 3


def hand_made():
    return (lax.axis_size("dp"), lax.axis_size("tensor")) == MESH_SHAPE


def device_rows_first(values):
    return values.transpose((0, 3, 4, 5, 1, 2) + tuple(range(6, values.ndim)))


def device_rows_last(values):
    return values.transpose((0, 4, 5, 1, 2, 3) + tuple(range(6, values.ndim)))


def gather_all(blocks, small, vectors):
    parts, depth = lax.axis_size("tensor"), lax.axis_size("dp")
    count, rows, columns = blocks.shape
    if hand_made():
        groups = (
            (((1, (0,), (), 0), (2, (), (), 1)),)
            + tuple(
                tuple((0, (at,), (half,), half) for half in range(ROW_HALVES))
                for at in range(count)
            )
            + (((1, (1,), (), 1),),)
        )
        halves = blocks.reshape(count, ROW_HALVES, rows // ROW_HALVES, columns)
        padded = jnp.pad(vectors, (0, -vectors.size % 1024)).reshape(-1, 128)
        wide, thin, lists = spread([halves, small, padded], groups, 1)
        thin = device_rows_first(thin)
        lists = lists[:, :, 0, 0, 0].reshape(parts, -1)[:, : vectors.size]
    else:
        both = ("dp", "tensor")
        wide = lax.all_gather(blocks, both, axis=0, tiled=False)
        wide = wide.reshape(depth, parts, count, rows, columns).transpose(2, 1, 0, 3, 4)
        thin = lax.all_gather(small, both, axis=1, tiled=True)
        lists = lax.all_gather(vectors, "tensor", axis=0, tiled=False)
    return (
        wide.reshape(count * parts, depth * rows, columns),
        thin.reshape(small.shape[0], -1, small.shape[-1]),
        lists,
    )


def sum_layer(attn_part, mlp_part):
    parts, depth = lax.axis_size("tensor"), lax.axis_size("dp")
    rows, columns = attn_part.shape[1] // depth, attn_part.shape[2]
    if hand_made():
        form = (2,) * len(DIMS) + (ROW_HALVES, rows // ROW_HALVES, columns)
        groups = tuple(
            tuple((1, (at,), (half,), half) for half in range(ROW_HALVES)) for at in range(2)
        ) + (tuple((0, (), (half,), half) for half in range(ROW_HALVES)),)
        attn_sum, mlp_sum = collect(
            [attn_part.reshape(form), mlp_part.reshape((2,) + form)], groups, 2
        )
    else:
        whole = jnp.concatenate([attn_part[None], mlp_part]).reshape(
            LAYER_BLOCKS, parts, depth, rows, columns
        )
        whole = whole.transpose(2, 1, 0, 3, 4).reshape(-1, LAYER_BLOCKS, rows, columns)
        total = lax.psum_scatter(
            whole, ("dp", "tensor"), scatter_dimension=0, tiled=False
        ).astype(jnp.float32)
        attn_sum, mlp_sum = total[0], total[1:]
    return attn_sum.reshape(rows, columns), mlp_sum.reshape(2, rows, columns)


def sum_small(small):
    devices = lax.axis_size("dp") * lax.axis_size("tensor")
    rows = small.shape[1] // devices
    if hand_made():
        form = device_rows_last(small.reshape((2,) + (2,) * len(DIMS) + (rows, SMALL_WIDTH)))
        groups = (tuple((0, (at,), (), at) for at in range(2)),)
        return collect([form], groups, 3)[0]
    blocks = small.reshape(2, devices, rows, -1).transpose(1, 0, 2, 3)
    return lax.psum_scatter(
        blocks, ("dp", "tensor"), scatter_dimension=0, tiled=False
    ).astype(jnp.float32)


def exchange_kernel(routes, *refs):
    count = len(routes)
    sources, totals = refs[:count], refs[count : 2 * count]
    landed = refs[2 * count : 3 * count]
    send_sem, recv_sem = refs[3 * count :]
    place = place_of_device()
    for source, total in zip(sources, totals):
        total[...] = source[...]
    meet_partners(place)
    for stage in range(max(len(route) for route in routes)):
        copies = []
        for index, route in enumerate(routes):
            if stage < len(route):
                copies.append(
                    (
                        index,
                        pltpu.make_async_remote_copy(
                            src_ref=totals[index],
                            dst_ref=landed[index].at[stage],
                            send_sem=send_sem.at[index, stage],
                            recv_sem=recv_sem.at[index, stage],
                            device_id=partner_of(place, route[stage]),
                            device_id_type=MESH,
                        ),
                    )
                )
        for _, copy in copies:
            copy.start()
        for index, copy in copies:
            copy.wait()
            totals[index][...] += landed[index][stage]


def exchange(arrays, routes, collective_id):
    depth = max(len(route) for route in routes)
    return pl.pallas_call(
        partial(exchange_kernel, routes),
        out_shape=[jax.ShapeDtypeStruct(member.shape, member.dtype) for member in arrays],
        in_specs=[pl.BlockSpec(memory_space=pltpu.VMEM)] * len(arrays),
        out_specs=[pl.BlockSpec(memory_space=pltpu.VMEM)] * len(arrays),
        scratch_shapes=[
            pltpu.VMEM((len(route),) + member.shape, member.dtype)
            for member, route in zip(arrays, routes)
        ]
        + [
            pltpu.SemaphoreType.DMA((len(arrays), depth)),
            pltpu.SemaphoreType.DMA((len(arrays), depth)),
        ],
        compiler_params=pltpu.CompilerParams(
            collective_id=collective_id, has_side_effects=True, vmem_limit_bytes=16 << 20
        ),
    )(*arrays)


ROUTES = {
    "both": ("c", "y", "x", "za", "zb"),
    "tensor": ("c", "y"),
    "dp": ("x", "za", "zb"),
}


def sums_over(requests, collective_id):
    if not hand_made():
        names = {"both": ("dp", "tensor"), "tensor": "tensor", "dp": "dp"}
        return [summed_over(names[axes], arrays) for axes, arrays in requests]
    packed = []
    for _, arrays in requests:
        flat = flatten_all(arrays)
        packed.append(jnp.pad(flat, (0, -flat.size % 1024)).reshape(-1, 128))
    totals = exchange(packed, tuple(ROUTES[axes] for axes, _ in requests), collective_id)
    return [
        split_all(total.reshape(-1), [member.shape for member in arrays])
        for total, (_, arrays) in zip(totals, requests)
    ]


def finish_step(weight, update, update_sq, weight_sq, entries):
    clip_factor = jnp.maximum(1.0, jnp.sqrt(update_sq / entries) / clip_level)
    step_size = step_ratio * jnp.maximum(floor_scale, jnp.sqrt(weight_sq / entries))
    return weight - step_size * update / clip_factor


def shards(
    patches, labels, image_count,
    attn_weight, attn_rows, attn_cols,
    mlp_weight, mlp_rows, mlp_cols,
    patch_weight, patch_rows, patch_cols,
    embed_table, embed_rows, embed_cols,
    head_weight, head_rows, head_cols,
    split_vec, split_sq, hidden_bias, hidden_sq,
    shared_vec, shared_sq, head_bias, head_bias_sq,
):
    both = ("dp", "tensor")
    low = jnp.bfloat16
    tensor_width = lax.axis_size("tensor")
    dp_width = lax.axis_size("dp")
    tensor_rank = lax.axis_index("tensor")
    shard_rank = lax.axis_index("dp")
    images = patches.shape[0]
    own_rows = attn_weight.shape[1]
    attn_width = attn_weight.shape[3]
    mlp_width = mlp_weight.shape[3]
    slot_index = tensor_rank * images + jnp.arange(images)
    image_total = jnp.sum(image_count).astype(jnp.float32)
    image_weight = (
        jnp.where(slot_index < image_count[shard_rank], 1.0, 0.0).astype(jnp.float32) / image_total
    )

    blocks = jnp.concatenate(
        [attn_weight.reshape(LAYERS, 1, own_rows, 4 * attn_width), mlp_weight], axis=1
    ).astype(low)
    widen = lambda values: jnp.pad(
        values, ((0, 0), (0, SMALL_WIDTH - values.shape[1]))
    )
    small = jnp.stack(
        [widen(jnp.concatenate([patch_weight, embed_table], axis=1)), widen(head_weight)]
    ).astype(low)
    weights, small_full, vectors = gather_all(
        blocks.reshape(LAYERS * LAYER_BLOCKS, own_rows, mlp_width),
        small,
        flatten_all([split_vec, hidden_bias]),
    )
    patch_full, table_full = small_full[0, :, :D], small_full[0, :, D : D + EXTRA]
    head_full = small_full[1, :, :CLASSES]
    split_rows = vectors[:, : split_vec.size].reshape(tensor_width, LAYERS, 2, attn_width)
    split_rows = jnp.stack(
        [split_rows[:, :, 0], jnp.zeros_like(split_rows[:, :, 0]), split_rows[:, :, 1]], axis=2
    ).reshape(tensor_width, LAYERS, 1, 3 * attn_width)
    hidden_rows = vectors[:, split_vec.size :].reshape(tensor_width, LAYERS, 1, mlp_width)

    table_rows = table_full.astype(jnp.float32).T
    pixel_rows = patches.reshape(images * (TOK_IMG - 1), PATCH)
    embedded = jnp.dot(pixel_rows, patch_full, preferred_element_type=jnp.float32).reshape(
        images, TOK_IMG - 1, D
    )
    embedded = embedded + table_rows[1:TOK_IMG] + table_rows[TOK_IMG]
    residual = jnp.concatenate(
        [
            jnp.broadcast_to(table_rows[0], (images, 1, D)),
            embedded,
            jnp.zeros((images, PAD_ROWS - TOK_IMG, D), jnp.float32),
        ],
        axis=1,
    ).reshape(images * PAD_ROWS, D)

    saved = []
    for layer_idx in range(LAYERS):
        gains = shared_vec[6 * layer_idx : 6 * layer_idx + 6]
        layer_input = residual
        residual, mid, qkv, mixed, act, slope = forward_layer(
            layer_idx, images, residual, gains, weights,
            split_rows[:, layer_idx], hidden_rows[:, layer_idx],
        )
        saved.append((layer_input, mid, gains, qkv, mixed, act, slope))
    cls_rows = residual.reshape(images, PAD_ROWS, D)[:, 0]
    feature, final_back = jax.vjp(
        layer_norm, cls_rows, shared_vec[6 * LAYERS], shared_vec[6 * LAYERS + 1]
    )
    feature_low = feature.astype(low)
    logits = jnp.dot(feature_low, head_full, preferred_element_type=jnp.float32) + head_bias
    log_norm = jax.nn.logsumexp(logits, axis=-1, keepdims=True)
    onehot = jnp.where(labels[:, None] == jnp.arange(CLASSES)[None, :], 1.0, 0.0).astype(
        jnp.float32
    )
    target = (1.0 - smoothing) * onehot + smoothing / CLASSES
    loss_part = jnp.sum((log_norm[:, 0] - jnp.sum(target * logits, axis=-1)) * image_weight)
    grad_logits = (jnp.exp(logits - log_norm) - target) * image_weight[:, None]
    grad_head_bias = jnp.sum(grad_logits, axis=0)
    logits_low = grad_logits.astype(low)
    grad_head = outer_sum(feature_low, logits_low)
    grad_feature = times_transposed(logits_low, head_full)
    grad_cls, grad_final_gain, grad_final_shift = final_back(grad_feature)
    grad_rows = jnp.concatenate(
        [grad_cls[:, None], jnp.zeros((images, PAD_ROWS - 1, D), jnp.float32)], axis=1
    ).reshape(images * PAD_ROWS, D)
    shared_list = [None] * LAYERS
    split_list = [None] * LAYERS
    hidden_list = [None] * LAYERS
    attn_list = [None] * LAYERS
    mlp_list = [None] * LAYERS
    for layer_idx in reversed(range(LAYERS)):
        layer_input, mid, gains, qkv, mixed, act, slope = saved[layer_idx]
        grad_rows, attn_part, mlp_part, shared_list[layer_idx], split_part, hidden_part = (
            backward_layer(
                layer_idx, images, grad_rows, layer_input, mid, gains, weights,
                qkv, mixed, act, slope,
            )
        )
        split_part = split_part.reshape(tensor_width, 3, attn_width)
        split_list[layer_idx] = jnp.stack([split_part[:, 0], split_part[:, 2]], axis=1)
        hidden_list[layer_idx] = hidden_part.reshape(tensor_width, mlp_width)
        attn_sum, mlp_list[layer_idx] = sum_layer(attn_part, mlp_part)
        attn_list[layer_idx] = attn_sum.reshape(own_rows, 4, attn_width)
    grad_image = grad_rows.reshape(images, PAD_ROWS, D)
    grad_first = jnp.sum(grad_image[:, 0], axis=0)
    grad_position = jnp.sum(grad_image[:, 1:TOK_IMG], axis=0)
    grad_patch_bias = jnp.sum(grad_position, axis=0)
    embed_low = grad_image[:, 1:TOK_IMG].astype(low).reshape(images * (TOK_IMG - 1), D)
    grad_patch = outer_sum(pixel_rows, embed_low)
    grad_table = jnp.concatenate([grad_first[None], grad_position, grad_patch_bias[None]], axis=0).T
    small_sum = sum_small(
        jnp.stack(
            [widen(jnp.concatenate([grad_patch, grad_table], axis=1)), widen(grad_head)]
        ).astype(low)
    )
    patch_grad, table_grad = small_sum[0, :, :D], small_sum[0, :, D : D + EXTRA]
    head_grad = small_sum[1, :, :CLASSES]
    attn_grad = jnp.stack(attn_list)
    mlp_grad = jnp.stack(mlp_list)
    shared_grad = jnp.concatenate(
        shared_list + [jnp.stack([grad_final_gain, grad_final_shift])], axis=0
    )
    attn_sq = attn_grad * attn_grad
    mlp_sq = mlp_grad * mlp_grad
    patch_sq = patch_grad * patch_grad
    table_sq = table_grad * table_grad
    head_sq = head_grad * head_grad

    split_sums, hidden_sums, shared_full, head_bias_full, loss_total = summed_over(
        both,
        [jnp.stack(split_list, 1), jnp.stack(hidden_list, 1), shared_grad, grad_head_bias, loss_part],
    )
    split_total = lax.dynamic_index_in_dim(split_sums, tensor_rank, 0, keepdims=False)
    hidden_total = lax.dynamic_index_in_dim(hidden_sums, tensor_rank, 0, keepdims=False)
    patch_row_new = decay_rate * patch_rows + (1.0 - decay_rate) * (
        jnp.sum(patch_sq, axis=1) / D + tiny_sq
    )
    table_row_new = decay_rate * embed_rows + (1.0 - decay_rate) * (
        jnp.sum(table_sq, axis=1) / EXTRA + tiny_sq
    )
    head_row_new = decay_rate * head_rows + (1.0 - decay_rate) * (
        jnp.sum(head_sq, axis=1) / CLASSES + tiny_sq
    )
    own_share = 1.0 / tensor_width
    (
        (
            patch_col_full, table_col_full, head_col_full, whole_row_sum,
            attn_old_sum, mlp_old_sum, attn_total, mlp_total, weight_sq_parts,
        ),
        (attn_row_full, mlp_row_full),
        (attn_col_full, mlp_col_full),
    ) = sums_over(
        [
            (
                "both",
                [
                    jnp.sum(patch_sq, axis=0),
                    jnp.sum(table_sq, axis=0),
                    jnp.sum(head_sq, axis=0),
                    jnp.stack(
                        [jnp.sum(patch_row_new), jnp.sum(table_row_new), jnp.sum(head_row_new)]
                    ),
                    jnp.sum(attn_rows, axis=-1) * own_share,
                    jnp.sum(mlp_rows, axis=-1) * own_share,
                    jnp.sum(attn_sq, axis=(1, 3)),
                    jnp.sum(mlp_sq, axis=(2, 3)),
                    flatten_all(
                        [
                            jnp.sum(attn_weight * attn_weight, axis=(1, 3)),
                            jnp.sum(mlp_weight * mlp_weight, axis=(2, 3)),
                            jnp.sum(patch_weight * patch_weight),
                            jnp.sum(embed_table * embed_table),
                            jnp.sum(head_weight * head_weight),
                        ]
                    ),
                ],
            ),
            ("tensor", [jnp.sum(attn_sq, axis=3).transpose(0, 2, 1), jnp.sum(mlp_sq, axis=3)]),
            ("dp", [jnp.sum(attn_sq, axis=1), jnp.sum(mlp_sq, axis=2)]),
        ],
        4,
    )
    attn_row_new = decay_rate * attn_rows + (1.0 - decay_rate) * (attn_row_full / D + tiny_sq)
    mlp_row_new = decay_rate * mlp_rows + (1.0 - decay_rate) * (mlp_row_full / FF + tiny_sq)
    weight_sq = split_all(weight_sq_parts, [(LAYERS, 4), (LAYERS, 2), (), (), ()])
    attn_row_mean = (
        decay_rate * attn_old_sum + (1.0 - decay_rate) * (attn_total / D + D * tiny_sq)
    ) / D
    mlp_row_mean = (
        decay_rate * mlp_old_sum + (1.0 - decay_rate) * (mlp_total / FF + D * tiny_sq)
    ) / D
    whole_row_mean = whole_row_sum / jnp.array([PATCH, D, D], jnp.float32)
    attn_col_new = decay_rate * attn_cols + (1.0 - decay_rate) * (attn_col_full / D + tiny_sq)
    mlp_col_new = decay_rate * mlp_cols + (1.0 - decay_rate) * (mlp_col_full / D + tiny_sq)
    patch_col_new = decay_rate * patch_cols + (1.0 - decay_rate) * (
        patch_col_full / PATCH + tiny_sq
    )
    table_col_new = decay_rate * embed_cols + (1.0 - decay_rate) * (table_col_full / D + tiny_sq)
    head_col_new = decay_rate * head_cols + (1.0 - decay_rate) * (head_col_full / D + tiny_sq)
    attn_update = attn_grad * lax.rsqrt(
        attn_row_new.transpose(0, 2, 1)[:, :, :, None]
        * attn_col_new[:, None]
        / attn_row_mean[:, None, :, None]
    )
    mlp_update = mlp_grad * lax.rsqrt(
        mlp_row_new[:, :, :, None] * mlp_col_new[:, :, None, :] / mlp_row_mean[:, :, None, None]
    )
    patch_update = patch_grad * lax.rsqrt(
        patch_row_new[:, None] * patch_col_new[None, :] / whole_row_mean[0]
    )
    table_update = table_grad * lax.rsqrt(
        table_row_new[:, None] * table_col_new[None, :] / whole_row_mean[1]
    )
    head_update = head_grad * lax.rsqrt(
        head_row_new[:, None] * head_col_new[None, :] / whole_row_mean[2]
    )
    split_sq_new = decay_rate * split_sq + (1.0 - decay_rate) * (
        split_total * split_total + tiny_sq
    )
    split_update = split_total * lax.rsqrt(split_sq_new)
    hidden_sq_new = decay_rate * hidden_sq + (1.0 - decay_rate) * (
        hidden_total * hidden_total + tiny_sq
    )
    hidden_update = hidden_total * lax.rsqrt(hidden_sq_new)
    shared_sq_new = decay_rate * shared_sq + (1.0 - decay_rate) * (
        shared_full * shared_full + tiny_sq
    )
    shared_update = shared_full * lax.rsqrt(shared_sq_new)
    head_bias_sq_new = decay_rate * head_bias_sq + (1.0 - decay_rate) * (
        head_bias_full * head_bias_full + tiny_sq
    )
    head_bias_update = head_bias_full * lax.rsqrt(head_bias_sq_new)
    dp_share = 1.0 / dp_width
    ((attn_u2, mlp_u2, patch_u2, table_u2, head_u2, split_u2, hidden_u2, split_w2, hidden_w2),) = (
        sums_over(
            [("both", [
                jnp.sum(attn_update * attn_update, axis=(1, 3)),
                jnp.sum(mlp_update * mlp_update, axis=(2, 3)),
                jnp.sum(patch_update * patch_update),
                jnp.sum(table_update * table_update),
                jnp.sum(head_update * head_update),
                jnp.sum(split_update * split_update, axis=-1) * dp_share,
                jnp.sum(hidden_update * hidden_update, axis=-1) * dp_share,
                jnp.sum(split_vec * split_vec, axis=-1) * dp_share,
                jnp.sum(hidden_bias * hidden_bias, axis=-1) * dp_share,
            ])],
            5,
        )
    )
    vector_sq = [split_w2, hidden_w2]
    attn_new = finish_step(
        attn_weight, attn_update, attn_u2[:, None, :, None], weight_sq[0][:, None, :, None], D * D
    )
    mlp_new = finish_step(
        mlp_weight, mlp_update, mlp_u2[:, :, None, None], weight_sq[1][:, :, None, None], D * FF
    )
    patch_new = finish_step(patch_weight, patch_update, patch_u2, weight_sq[2], PATCH * D)
    embed_new = finish_step(embed_table, table_update, table_u2, weight_sq[3], D * EXTRA)
    head_new = finish_step(head_weight, head_update, head_u2, weight_sq[4], D * CLASSES)
    split_new = finish_step(
        split_vec, split_update, split_u2[:, :, None], vector_sq[0][:, :, None], D
    )
    hidden_new = finish_step(
        hidden_bias, hidden_update, hidden_u2[:, None], vector_sq[1][:, None], FF
    )
    shared_new = finish_step(
        shared_vec,
        shared_update,
        jnp.sum(shared_update * shared_update, axis=-1, keepdims=True),
        jnp.sum(shared_vec * shared_vec, axis=-1, keepdims=True),
        D,
    )
    head_bias_new = finish_step(
        head_bias,
        head_bias_update,
        jnp.sum(head_bias_update * head_bias_update),
        jnp.sum(head_bias * head_bias),
        CLASSES,
    )
    return (
        loss_total,
        attn_new,
        attn_row_new,
        attn_col_new,
        mlp_new,
        mlp_row_new,
        mlp_col_new,
        patch_new,
        patch_row_new,
        patch_col_new,
        embed_new,
        table_row_new,
        table_col_new,
        head_new,
        head_row_new,
        head_col_new,
        split_new,
        split_sq_new,
        hidden_new,
        hidden_sq_new,
        shared_new,
        shared_sq_new,
        head_bias_new,
        head_bias_sq_new,
    )


def solution(mesh):
    in_specs = (
        P(("dp", "tensor"), None, None),
        P(("dp", "tensor")),
        P(),
        P(None, "dp", None, "tensor"),
        P(None, None, "dp"),
        P(None, None, "tensor"),
        P(None, None, "dp", "tensor"),
        P(None, None, "dp"),
        P(None, None, "tensor"),
        P(("dp", "tensor"), None),
        P(("dp", "tensor")),
        P(),
        P(("dp", "tensor"), None),
        P(("dp", "tensor")),
        P(),
        P(("dp", "tensor"), None),
        P(("dp", "tensor")),
        P(),
        P(None, None, "tensor"),
        P(None, None, "tensor"),
        P(None, "tensor"),
        P(None, "tensor"),
        P(),
        P(),
        P(),
        P(),
    )
    out_specs = (
        P(),
        P(None, "dp", None, "tensor"),
        P(None, None, "dp"),
        P(None, None, "tensor"),
        P(None, None, "dp", "tensor"),
        P(None, None, "dp"),
        P(None, None, "tensor"),
        P(("dp", "tensor"), None),
        P(("dp", "tensor")),
        P(),
        P(("dp", "tensor"), None),
        P(("dp", "tensor")),
        P(),
        P(("dp", "tensor"), None),
        P(("dp", "tensor")),
        P(),
        P(None, None, "tensor"),
        P(None, None, "tensor"),
        P(None, "tensor"),
        P(None, "tensor"),
        P(),
        P(),
        P(),
        P(),
    )
    return jax.shard_map(shards, mesh=mesh, in_specs=in_specs, out_specs=out_specs, check_vma=False)
```

```python
from functools import partial
import math

import jax
import jax.numpy as jnp
from jax import lax
from jax.experimental import pallas as pl
from jax.experimental.pallas import tpu as pltpu
from jax.sharding import PartitionSpec as P

D = 768
HEAD_DIM = 64
FF = 3072
PATCH = 768
CLASSES = 1000
TOK_IMG = 197
LAYERS = 3
SEQ = 200
EXTRA = 198


decay_rate = 0.5
tiny_sq = 1e-30
floor_scale = 0.001
step_ratio = 1.0
clip_level = 0.1
smoothing = 0.1
norm_eps = 1e-06


def layer_norm(values, gain_vec, shift_vec):
    centred = values - jnp.mean(values, axis=-1, keepdims=True)
    spread = jnp.mean(centred * centred, axis=-1, keepdims=True)
    return centred * lax.rsqrt(spread + norm_eps) * gain_vec + shift_vec


def outer_sum(left_rows, right_rows):
    return lax.dot_general(
        left_rows, right_rows, (((0,), (0,)), ((), ())), preferred_element_type=jnp.float32
    )


def times_transposed(left_rows, right_matrix):
    return lax.dot_general(
        left_rows, right_matrix, (((1,), (1,)), ((), ())), preferred_element_type=jnp.float32
    )


def flatten_all(arrays):
    return jnp.concatenate([jnp.ravel(member) for member in arrays])


def split_all(flat, shapes):
    outputs = []
    offset = 0
    for form_shape in shapes:
        length = math.prod(form_shape)
        outputs.append(flat[offset : offset + length].reshape(form_shape))
        offset = offset + length
    return outputs


def summed_over(axes, arrays):
    return split_all(
        lax.psum(flatten_all(arrays), axes), [member.shape for member in arrays]
    )


MESH = pl.DeviceIdType.MESH
DIMS = ("y", "c", "zb", "za", "x")
OUT_ORDERS = (("zb", "x", "za", "y", "c"), ("zb", "y", "za", "x", "c"))
IN_ORDERS = tuple(order[::-1] for order in OUT_ORDERS)


def place_of_device():
    dp, tensor = lax.axis_index("dp"), lax.axis_index("tensor")
    return {
        "x": lax.rem(dp, 2),
        "za": lax.rem(dp // 2, 2),
        "zb": dp // 4,
        "y": tensor // 2,
        "c": lax.rem(tensor, 2),
    }


def partner_of(place, dim):
    moved = dict(place)
    moved[dim] = 1 - place[dim]
    return (
        moved["zb"] * 4 + moved["za"] * 2 + moved["x"],
        moved["y"] * 2 + moved["c"],
    )


def meet_partners(place):
    barrier = pltpu.get_barrier_semaphore()
    for dim in DIMS:
        pl.semaphore_signal(
            barrier, inc=1, device_id=partner_of(place, dim), device_id_type=MESH
        )
    pl.semaphore_wait(barrier, len(DIMS))


def spread_kernel(groups, *refs):
    arrays = len({flow[0] for group in groups for flow in group})
    sources, targets = refs[:arrays], refs[arrays : 2 * arrays]
    send_sem, recv_sem, own_sem = refs[2 * arrays :]
    place = place_of_device()
    flows = [flow for group in groups for flow in group]
    number = {flow: position for position, flow in enumerate(flows)}

    def own_copy(flow):
        array, lead, tail, _ = flow
        slot = lead + tuple(place[dim] for dim in DIMS) + tail
        return pltpu.make_async_copy(
            sources[array].at[lead + tail], targets[array].at[slot], own_sem.at[number[flow]]
        )

    def stage_copy(flow, stage):
        array, lead, tail, order = flow
        dims = OUT_ORDERS[order]
        done = dims[:stage]
        slot = lead + tuple(slice(None) if dim in done else place[dim] for dim in DIMS) + tail
        source = sources[array].at[lead + tail] if stage == 0 else targets[array].at[slot]
        return pltpu.make_async_remote_copy(
            src_ref=source,
            dst_ref=targets[array].at[slot],
            send_sem=send_sem.at[number[flow], stage],
            recv_sem=recv_sem.at[number[flow], stage],
            device_id=partner_of(place, dims[stage]),
            device_id_type=MESH,
        )

    meet_partners(place)
    stages = len(DIMS)
    for tick in range(len(groups) + stages):
        for stage in reversed(range(stages + 1)):
            if not 0 <= tick - stage < len(groups):
                continue
            for flow in groups[tick - stage]:
                if stage == 1:
                    own_copy(flow).wait()
                if stage > 0:
                    stage_copy(flow, stage - 1).wait_recv()
                if stage == 0:
                    own_copy(flow).start()
                if stage < stages:
                    stage_copy(flow, stage).start()
    for flow in flows:
        for stage in range(stages):
            stage_copy(flow, stage).wait_send()


def spread(arrays, groups, collective_id):
    count = sum(len(group) for group in groups)
    leads = {flow[0]: len(flow[1]) for group in groups for flow in group}
    shapes = [
        member.shape[: leads[position]] + (2,) * len(DIMS) + member.shape[leads[position] :]
        for position, member in enumerate(arrays)
    ]
    return pl.pallas_call(
        partial(spread_kernel, groups),
        out_shape=[
            jax.ShapeDtypeStruct(shape, member.dtype) for shape, member in zip(shapes, arrays)
        ],
        in_specs=[pl.BlockSpec(memory_space=pltpu.VMEM)] * len(arrays),
        out_specs=[pl.BlockSpec(memory_space=pl.ANY)] * len(arrays),
        scratch_shapes=[
            pltpu.SemaphoreType.DMA((count, len(DIMS))),
            pltpu.SemaphoreType.DMA((count, len(DIMS))),
            pltpu.SemaphoreType.DMA((count,)),
        ],
        compiler_params=pltpu.CompilerParams(
            collective_id=collective_id, has_side_effects=True, vmem_limit_bytes=16 << 20
        ),
    )(*arrays)


def collect_kernel(groups, arrays, *refs):
    sources, targets = refs[:arrays], refs[arrays : 2 * arrays]
    held, landed = refs[2 * arrays], refs[2 * arrays + 1 : 2 * arrays + 6]
    send_sem, recv_sem, own_sem = refs[2 * arrays + 6 :]
    place = place_of_device()
    flows = [flow for group in groups for flow in group]
    number = {flow: position for position, flow in enumerate(flows)}
    kept = ("y", "zb", "za", "x")

    def core_slot(flow, core):
        _, lead, tail, _ = flow
        return lead + tuple(core if dim == "c" else slice(None) for dim in DIMS) + tail

    def own_copy(flow):
        return pltpu.make_async_copy(
            sources[flow[0]].at[core_slot(flow, place["c"])],
            held.at[number[flow]],
            own_sem.at[number[flow]],
        )

    def held_slot(done, moved):
        slot = ()
        for dim in kept:
            if dim == moved:
                slot += (1 - place[dim],)
            elif dim in done:
                slot += (place[dim],)
            else:
                slot += (slice(None),)
        return slot

    def stage_copy(flow, stage):
        dims = IN_ORDERS[flow[3]]
        index = number[flow]
        if stage == 0:
            source = sources[flow[0]].at[core_slot(flow, 1 - place["c"])]
        else:
            source = held.at[(index,) + held_slot(dims[:stage], dims[stage])]
        return pltpu.make_async_remote_copy(
            src_ref=source,
            dst_ref=landed[stage].at[index],
            send_sem=send_sem.at[index, stage],
            recv_sem=recv_sem.at[index, stage],
            device_id=partner_of(place, dims[stage]),
            device_id_type=MESH,
        )

    def add_landed(flow, stage):
        array, lead, tail, order = flow
        dims = IN_ORDERS[order]
        index = number[flow]
        free = [dim for dim in kept if dim not in dims[: stage + 1]]

        def add_block(step, carry):
            rest = step
            at = {}
            for dim in reversed(free):
                at[dim] = lax.rem(rest, 2)
                rest = rest // 2
            slot = (index,) + tuple(at[dim] if dim in free else place[dim] for dim in kept)
            landed_slot = (index,) + tuple(at[dim] for dim in free)
            total = held[slot].astype(jnp.float32) + landed[stage][landed_slot].astype(jnp.float32)
            if stage == len(DIMS) - 1:
                targets[array][lead + tail] = total
            else:
                held[slot] = total.astype(jnp.bfloat16)
            return carry

        if free:
            lax.fori_loop(0, 2 ** len(free), add_block, 0)
        else:
            add_block(0, 0)

    meet_partners(place)
    stages = len(DIMS)
    for tick in range(len(groups) + stages):
        for stage in reversed(range(stages + 1)):
            if not 0 <= tick - stage < len(groups):
                continue
            for flow in groups[tick - stage]:
                if stage == 0:
                    own_copy(flow).start()
                if stage == 1:
                    own_copy(flow).wait()
                if stage > 0:
                    stage_copy(flow, stage - 1).wait_recv()
                    add_landed(flow, stage - 1)
                if stage < stages:
                    stage_copy(flow, stage).start()
    for flow in flows:
        for stage in range(stages):
            stage_copy(flow, stage).wait_send()


def collect(arrays, groups, collective_id):
    leads = {flow[0]: len(flow[1]) for group in groups for flow in group}
    count = sum(len(group) for group in groups)
    block = arrays[0].shape[-2:]
    low = jnp.bfloat16
    return pl.pallas_call(
        partial(collect_kernel, groups, len(arrays)),
        out_shape=[
            jax.ShapeDtypeStruct(
                member.shape[: leads[position]] + member.shape[leads[position] + len(DIMS) :],
                jnp.float32,
            )
            for position, member in enumerate(arrays)
        ],
        in_specs=[pl.BlockSpec(memory_space=pl.ANY)] * len(arrays),
        out_specs=[pl.BlockSpec(memory_space=pltpu.VMEM)] * len(arrays),
        scratch_shapes=[
            pltpu.VMEM((count, 2, 2, 2, 2) + block, low),
            pltpu.VMEM((count, 2, 2, 2, 2) + block, low),
            pltpu.VMEM((count, 2, 2, 2) + block, low),
            pltpu.VMEM((count, 2, 2) + block, low),
            pltpu.VMEM((count, 2) + block, low),
            pltpu.VMEM((count,) + block, low),
            pltpu.SemaphoreType.DMA((count, len(DIMS))),
            pltpu.SemaphoreType.DMA((count, len(DIMS))),
            pltpu.SemaphoreType.DMA((count,)),
        ],
        compiler_params=pltpu.CompilerParams(
            collective_id=collective_id, has_side_effects=True, vmem_limit_bytes=67043328
        ),
    )(*arrays)


PAD_ROWS = 208
HALF_ROOT = 0.7071067811865476
DENSITY = 0.3989422804014327


def dot_nn(left, right):
    return lax.dot_general(left, right, (((1,), (0,)), ((), ())), preferred_element_type=jnp.float32)


def dot_nt(left, right):
    return lax.dot_general(left, right, (((1,), (1,)), ((), ())), preferred_element_type=jnp.float32)


def dot_tn(left, right):
    return lax.dot_general(left, right, (((0,), (0,)), ((), ())), preferred_element_type=jnp.float32)


def normal_form(values):
    centred = values - jnp.mean(values, axis=-1, keepdims=True)
    spread_sq = jnp.mean(centred * centred, axis=-1, keepdims=True)
    inverse = lax.rsqrt(spread_sq + norm_eps)
    return centred * inverse, inverse


def norm_back(grad, unit, inverse, gain):
    inner = grad * gain
    return inverse * (
        inner
        - jnp.mean(inner, axis=-1, keepdims=True)
        - unit * jnp.mean(inner * unit, axis=-1, keepdims=True)
    )


def head_probs(query, key):
    scores = dot_nt(query, key) * HEAD_DIM ** (-0.5)
    column = lax.broadcasted_iota(jnp.int32, scores.shape, 1)
    scores = jnp.where(column < TOK_IMG, scores, -1e30)
    powers = jnp.exp(scores - jnp.max(scores, axis=-1, keepdims=True))
    return powers / jnp.sum(powers, axis=-1, keepdims=True)


def forward_kernel(
    images, parts, x_ref, gain_ref, attn_ref, up_ref, down_ref, split_ref, hidden_ref,
    next_ref, mid_ref, qkv_ref, mixed_ref, act_ref, slope_ref, normed,
):
    step = pl.program_id(0)
    low = jnp.bfloat16
    width = mixed_ref.shape[-1]
    heads = width // HEAD_DIM

    @pl.when(step == 0)
    def _():
        unit, _ = normal_form(x_ref[...])
        normed[...] = (unit * gain_ref[0:1] + gain_ref[1:2]).astype(low)
        mid_ref[...] = x_ref[...] + gain_ref[2:3]

    @pl.when(step < parts)
    def _():
        weights = attn_ref[0]
        qkv = (dot_nn(normed[...], weights[:, : 3 * width]) + split_ref[0]).astype(low)
        qkv_ref[0] = qkv
        columns = []
        for head in range(heads):
            rows = []
            for image in range(images):
                at = slice(image * PAD_ROWS, (image + 1) * PAD_ROWS)
                query, key, value = (
                    qkv[at, kind * width + head * HEAD_DIM : kind * width + (head + 1) * HEAD_DIM]
                    for kind in range(3)
                )
                probs = head_probs(query, key).astype(low)
                rows.append(dot_nn(probs, value).astype(low))
            columns.append(jnp.concatenate(rows, axis=0))
        mixed = jnp.concatenate(columns, axis=1)
        mixed_ref[0] = mixed
        mid_ref[...] += dot_nt(mixed, weights[:, 3 * width :])

    @pl.when(step == parts)
    def _():
        unit, _ = normal_form(mid_ref[...])
        normed[...] = (unit * gain_ref[3:4] + gain_ref[4:5]).astype(low)
        next_ref[...] = mid_ref[...] + gain_ref[5:6]

    @pl.when(step >= parts)
    def _():
        pre = dot_nn(normed[...], up_ref[0]) + hidden_ref[0]
        share = 0.5 * (1.0 + lax.erf(pre * HALF_ROOT))
        act = (pre * share).astype(low)
        act_ref[0] = act
        slope_ref[0] = (share + pre * (DENSITY * jnp.exp(-0.5 * pre * pre))).astype(low)
        next_ref[...] += dot_nt(act, down_ref[0])


def forward_layer(layer_idx, images, x, gains, weights, split_rows, hidden_rows):
    rows = x.shape[0]
    parts = hidden_rows.shape[0]
    base = layer_idx * 3 * parts
    width, hidden = split_rows.shape[-1] // 3, hidden_rows.shape[-1]
    block = weights.shape[1:]
    early = lambda step: jnp.minimum(step, parts - 1)
    late = lambda step: jnp.maximum(step - parts, 0)
    whole = lambda shape: pl.BlockSpec(shape, lambda step: (0,) * len(shape))
    low = jnp.bfloat16
    return pl.pallas_call(
        partial(forward_kernel, images, parts),
        grid=(2 * parts,),
        out_shape=[
            jax.ShapeDtypeStruct((rows, D), jnp.float32),
            jax.ShapeDtypeStruct((rows, D), jnp.float32),
            jax.ShapeDtypeStruct((parts, rows, 3 * width), low),
            jax.ShapeDtypeStruct((parts, rows, width), low),
            jax.ShapeDtypeStruct((parts, rows, hidden), low),
            jax.ShapeDtypeStruct((parts, rows, hidden), low),
        ],
        in_specs=[
            whole((rows, D)),
            whole(gains.shape),
            pl.BlockSpec((1,) + block, lambda step: (base + early(step), 0, 0)),
            pl.BlockSpec((1,) + block, lambda step: (base + parts + late(step), 0, 0)),
            pl.BlockSpec((1,) + block, lambda step: (base + 2 * parts + late(step), 0, 0)),
            pl.BlockSpec((1, 1, 3 * width), lambda step: (early(step), 0, 0)),
            pl.BlockSpec((1, 1, hidden), lambda step: (late(step), 0, 0)),
        ],
        out_specs=[
            whole((rows, D)),
            whole((rows, D)),
            pl.BlockSpec((1, rows, 3 * width), lambda step: (early(step), 0, 0)),
            pl.BlockSpec((1, rows, width), lambda step: (early(step), 0, 0)),
            pl.BlockSpec((1, rows, hidden), lambda step: (late(step), 0, 0)),
            pl.BlockSpec((1, rows, hidden), lambda step: (late(step), 0, 0)),
        ],
        scratch_shapes=[pltpu.VMEM((rows, D), low)],
        compiler_params=pltpu.CompilerParams(vmem_limit_bytes=48 << 20),
    )(x, gains, weights, weights, weights, split_rows, hidden_rows)


def backward_kernel(
    images, parts, grad_ref, x_ref, mid_ref, gain_ref, attn_ref, up_ref, down_ref,
    qkv_ref, mixed_ref, act_ref, slope_ref,
    out_ref, attn_grad_ref, mlp_grad_ref, shared_ref, split_ref, hidden_ref,
    total, low_grad, turned_grad, turned_in,
):
    step = pl.program_id(0)
    low = jnp.bfloat16
    width = mixed_ref.shape[-1]
    heads = width // HEAD_DIM

    def row_sum(values):
        return jnp.sum(values, axis=0, keepdims=True)

    @pl.when(step == 0)
    def _():
        grad = grad_ref[...]
        shared_ref[5:6] = row_sum(grad)
        low_grad[...] = grad.astype(low)
        turned_grad[...] = grad.T.astype(low)
        unit, _ = normal_form(mid_ref[...])
        turned_in[...] = (unit * gain_ref[3:4] + gain_ref[4:5]).T.astype(low)
        total[...] = jnp.zeros_like(total)

    @pl.when(step < parts)
    def _():
        act_grad = dot_nn(low_grad[...], down_ref[0])
        mlp_grad_ref[1, 0] = dot_nn(turned_grad[...], act_ref[0]).astype(low)
        pre_grad = act_grad * slope_ref[0].astype(jnp.float32)
        hidden_ref[0] = row_sum(pre_grad)
        pre_low = pre_grad.astype(low)
        mlp_grad_ref[0, 0] = dot_nn(turned_in[...], pre_low).astype(low)
        total[...] += dot_nt(pre_low, up_ref[0])

    @pl.when(step == parts)
    def _():
        unit, inverse = normal_form(mid_ref[...])
        back = total[...]
        shared_ref[3:4] = row_sum(back * unit)
        shared_ref[4:5] = row_sum(back)
        grad = grad_ref[...] + norm_back(back, unit, inverse, gain_ref[3:4])
        out_ref[...] = grad
        shared_ref[2:3] = row_sum(grad)
        low_grad[...] = grad.astype(low)
        turned_grad[...] = grad.T.astype(low)
        unit, _ = normal_form(x_ref[...])
        turned_in[...] = (unit * gain_ref[0:1] + gain_ref[1:2]).T.astype(low)
        total[...] = jnp.zeros_like(total)

    @pl.when(step >= parts)
    def _():
        weights = attn_ref[0]
        qkv = qkv_ref[0]
        mixed_grad = dot_nn(low_grad[...], weights[:, 3 * width :]).astype(low)
        pieces = [[None] * heads for _ in range(3)]
        for head in range(heads):
            rows = [[], [], []]
            for image in range(images):
                at = slice(image * PAD_ROWS, (image + 1) * PAD_ROWS)
                query, key, value = (
                    qkv[at, kind * width + head * HEAD_DIM : kind * width + (head + 1) * HEAD_DIM]
                    for kind in range(3)
                )
                out_grad = mixed_grad[at, head * HEAD_DIM : (head + 1) * HEAD_DIM]
                probs = head_probs(query, key)
                prob_grad = dot_nt(out_grad, value)
                inner = jnp.sum(probs * prob_grad, axis=-1, keepdims=True)
                score_grad = (probs * (prob_grad - inner) * HEAD_DIM ** (-0.5)).astype(low)
                rows[0].append(dot_nn(score_grad, key))
                rows[1].append(dot_tn(score_grad, query))
                rows[2].append(dot_tn(probs.astype(low), out_grad))
            for kind in range(3):
                pieces[kind][head] = jnp.concatenate(rows[kind], axis=0)
        qkv_grad = jnp.concatenate(pieces[0] + pieces[1] + pieces[2], axis=1)
        split_ref[0] = row_sum(qkv_grad)
        qkv_low = qkv_grad.astype(low)
        attn_grad_ref[0, :, : 3 * width] = dot_nn(turned_in[...], qkv_low).astype(low)
        attn_grad_ref[0, :, 3 * width :] = dot_nn(turned_grad[...], mixed_ref[0]).astype(low)
        total[...] += dot_nt(qkv_low, weights[:, : 3 * width])

    @pl.when(step == 2 * parts - 1)
    def _():
        unit, inverse = normal_form(x_ref[...])
        back = total[...]
        shared_ref[0:1] = row_sum(back * unit)
        shared_ref[1:2] = row_sum(back)
        out_ref[...] += norm_back(back, unit, inverse, gain_ref[0:1])


def backward_layer(layer_idx, images, grad, x, mid, gains, weights, qkv, mixed, act, slope):
    rows = x.shape[0]
    parts = act.shape[0]
    base = layer_idx * 3 * parts
    width, hidden = mixed.shape[-1], act.shape[-1]
    block = weights.shape[1:]
    early = lambda step: jnp.minimum(step, parts - 1)
    late = lambda step: jnp.maximum(step - parts, 0)
    whole = lambda shape: pl.BlockSpec(shape, lambda step: (0,) * len(shape))
    low = jnp.bfloat16
    return pl.pallas_call(
        partial(backward_kernel, images, parts),
        grid=(2 * parts,),
        out_shape=[
            jax.ShapeDtypeStruct((rows, D), jnp.float32),
            jax.ShapeDtypeStruct((parts,) + block, low),
            jax.ShapeDtypeStruct((2, parts) + block, low),
            jax.ShapeDtypeStruct((6, D), jnp.float32),
            jax.ShapeDtypeStruct((parts, 1, 3 * width), jnp.float32),
            jax.ShapeDtypeStruct((parts, 1, hidden), jnp.float32),
        ],
        in_specs=[
            whole((rows, D)),
            whole((rows, D)),
            whole((rows, D)),
            whole(gains.shape),
            pl.BlockSpec((1,) + block, lambda step: (base + late(step), 0, 0)),
            pl.BlockSpec((1,) + block, lambda step: (base + parts + early(step), 0, 0)),
            pl.BlockSpec((1,) + block, lambda step: (base + 2 * parts + early(step), 0, 0)),
            pl.BlockSpec((1, rows, 3 * width), lambda step: (late(step), 0, 0)),
            pl.BlockSpec((1, rows, width), lambda step: (late(step), 0, 0)),
            pl.BlockSpec((1, rows, hidden), lambda step: (early(step), 0, 0)),
            pl.BlockSpec((1, rows, hidden), lambda step: (early(step), 0, 0)),
        ],
        out_specs=[
            whole((rows, D)),
            pl.BlockSpec((1,) + block, lambda step: (late(step), 0, 0)),
            pl.BlockSpec((2, 1) + block, lambda step: (0, early(step), 0, 0)),
            whole((6, D)),
            pl.BlockSpec((1, 1, 3 * width), lambda step: (late(step), 0, 0)),
            pl.BlockSpec((1, 1, hidden), lambda step: (early(step), 0, 0)),
        ],
        scratch_shapes=[
            pltpu.VMEM((rows, D), jnp.float32),
            pltpu.VMEM((rows, D), low),
            pltpu.VMEM((D, rows), low),
            pltpu.VMEM((D, rows), low),
        ],
        compiler_params=pltpu.CompilerParams(vmem_limit_bytes=56 << 20),
    )(grad, x, mid, gains, weights, weights, weights, qkv, mixed, act, slope)


MESH_SHAPE = (8, 4)
ROW_HALVES = 2
SMALL_WIDTH = 1024
LAYER_BLOCKS = 3


def hand_made():
    return (lax.axis_size("dp"), lax.axis_size("tensor")) == MESH_SHAPE


def device_rows_first(values):
    return values.transpose((0, 3, 4, 5, 1, 2) + tuple(range(6, values.ndim)))


def device_rows_last(values):
    return values.transpose((0, 4, 5, 1, 2, 3) + tuple(range(6, values.ndim)))


def gather_all(blocks, small, vectors):
    parts, depth = lax.axis_size("tensor"), lax.axis_size("dp")
    count, rows, columns = blocks.shape
    if hand_made():
        groups = (
            (((1, (0,), (), 0), (2, (), (), 1)),)
            + tuple(
                tuple((0, (at,), (half,), half) for half in range(ROW_HALVES))
                for at in range(count)
            )
            + (((1, (1,), (), 1),),)
        )
        halves = blocks.reshape(count, ROW_HALVES, rows // ROW_HALVES, columns)
        padded = jnp.pad(vectors, (0, -vectors.size % 1024)).reshape(-1, 128)
        wide, thin, lists = spread([halves, small, padded], groups, 1)
        thin = device_rows_first(thin)
        lists = lists[:, :, 0, 0, 0].reshape(parts, -1)[:, : vectors.size]
    else:
        both = ("dp", "tensor")
        wide = lax.all_gather(blocks, both, axis=0, tiled=False)
        wide = wide.reshape(depth, parts, count, rows, columns).transpose(2, 1, 0, 3, 4)
        thin = lax.all_gather(small, both, axis=1, tiled=True)
        lists = lax.all_gather(vectors, "tensor", axis=0, tiled=False)
    return (
        wide.reshape(count * parts, depth * rows, columns),
        thin.reshape(small.shape[0], -1, small.shape[-1]),
        lists,
    )


def sum_layers(pairs):
    parts, depth = lax.axis_size("tensor"), lax.axis_size("dp")
    rows, columns = pairs[0][0].shape[1] // depth, pairs[0][0].shape[2]
    sums = []
    if hand_made():
        form = (2,) * len(DIMS) + (ROW_HALVES, rows // ROW_HALVES, columns)
        arrays, groups = [], []
        for attn_part, mlp_part in pairs:
            position = len(arrays)
            arrays += [attn_part.reshape(form), mlp_part.reshape((2,) + form)]
            for at in range(2):
                groups.append(
                    tuple((position + 1, (at,), (half,), half) for half in range(ROW_HALVES))
                )
            groups.append(tuple((position, (), (half,), half) for half in range(ROW_HALVES)))
        totals = collect(arrays, tuple(groups), 2)
        for index in range(len(pairs)):
            attn_sum, mlp_sum = totals[2 * index : 2 * index + 2]
            sums.append((attn_sum.reshape(rows, columns), mlp_sum.reshape(2, rows, columns)))
        return sums
    for attn_part, mlp_part in pairs:
        whole = jnp.concatenate([attn_part[None], mlp_part]).reshape(
            LAYER_BLOCKS, parts, depth, rows, columns
        )
        whole = whole.transpose(2, 1, 0, 3, 4).reshape(-1, LAYER_BLOCKS, rows, columns)
        total = lax.psum_scatter(
            whole, ("dp", "tensor"), scatter_dimension=0, tiled=False
        ).astype(jnp.float32)
        sums.append((total[0], total[1:]))
    return sums


def sum_small(small):
    devices = lax.axis_size("dp") * lax.axis_size("tensor")
    rows = small.shape[1] // devices
    if hand_made():
        form = device_rows_last(small.reshape((2,) + (2,) * len(DIMS) + (rows, SMALL_WIDTH)))
        groups = (tuple((0, (at,), (), at) for at in range(2)),)
        return collect([form], groups, 3)[0]
    blocks = small.reshape(2, devices, rows, -1).transpose(1, 0, 2, 3)
    return lax.psum_scatter(
        blocks, ("dp", "tensor"), scatter_dimension=0, tiled=False
    ).astype(jnp.float32)


def exchange_kernel(routes, *refs):
    count = len(routes)
    sources, totals = refs[:count], refs[count : 2 * count]
    landed = refs[2 * count : 3 * count]
    send_sem, recv_sem = refs[3 * count :]
    place = place_of_device()
    for source, total in zip(sources, totals):
        total[...] = source[...]
    meet_partners(place)
    for stage in range(max(len(route) for route in routes)):
        copies = []
        for index, route in enumerate(routes):
            if stage < len(route):
                copies.append(
                    (
                        index,
                        pltpu.make_async_remote_copy(
                            src_ref=totals[index],
                            dst_ref=landed[index].at[stage],
                            send_sem=send_sem.at[index, stage],
                            recv_sem=recv_sem.at[index, stage],
                            device_id=partner_of(place, route[stage]),
                            device_id_type=MESH,
                        ),
                    )
                )
        for _, copy in copies:
            copy.start()
        for index, copy in copies:
            copy.wait()
            totals[index][...] += landed[index][stage]


def exchange(arrays, routes, collective_id):
    depth = max(len(route) for route in routes)
    return pl.pallas_call(
        partial(exchange_kernel, routes),
        out_shape=[jax.ShapeDtypeStruct(member.shape, member.dtype) for member in arrays],
        in_specs=[pl.BlockSpec(memory_space=pltpu.VMEM)] * len(arrays),
        out_specs=[pl.BlockSpec(memory_space=pltpu.VMEM)] * len(arrays),
        scratch_shapes=[
            pltpu.VMEM((len(route),) + member.shape, member.dtype)
            for member, route in zip(arrays, routes)
        ]
        + [
            pltpu.SemaphoreType.DMA((len(arrays), depth)),
            pltpu.SemaphoreType.DMA((len(arrays), depth)),
        ],
        compiler_params=pltpu.CompilerParams(
            collective_id=collective_id, has_side_effects=True, vmem_limit_bytes=16 << 20
        ),
    )(*arrays)


ROUTES = {
    "both": ("c", "y", "x", "za", "zb"),
    "tensor": ("c", "y"),
    "dp": ("x", "za", "zb"),
}


def sums_over(requests, collective_id):
    if not hand_made():
        names = {"both": ("dp", "tensor"), "tensor": "tensor", "dp": "dp"}
        return [summed_over(names[axes], arrays) for axes, arrays in requests]
    packed = []
    for _, arrays in requests:
        flat = flatten_all(arrays)
        packed.append(jnp.pad(flat, (0, -flat.size % 1024)).reshape(-1, 128))
    totals = exchange(packed, tuple(ROUTES[axes] for axes, _ in requests), collective_id)
    return [
        split_all(total.reshape(-1), [member.shape for member in arrays])
        for total, (_, arrays) in zip(totals, requests)
    ]


def finish_step(weight, update, update_sq, weight_sq, entries):
    clip_factor = jnp.maximum(1.0, jnp.sqrt(update_sq / entries) / clip_level)
    step_size = step_ratio * jnp.maximum(floor_scale, jnp.sqrt(weight_sq / entries))
    return weight - step_size * update / clip_factor


def shards(
    patches, labels, image_count,
    attn_weight, attn_rows, attn_cols,
    mlp_weight, mlp_rows, mlp_cols,
    patch_weight, patch_rows, patch_cols,
    embed_table, embed_rows, embed_cols,
    head_weight, head_rows, head_cols,
    split_vec, split_sq, hidden_bias, hidden_sq,
    shared_vec, shared_sq, head_bias, head_bias_sq,
):
    both = ("dp", "tensor")
    low = jnp.bfloat16
    tensor_width = lax.axis_size("tensor")
    dp_width = lax.axis_size("dp")
    tensor_rank = lax.axis_index("tensor")
    shard_rank = lax.axis_index("dp")
    images = patches.shape[0]
    own_rows = attn_weight.shape[1]
    attn_width = attn_weight.shape[3]
    mlp_width = mlp_weight.shape[3]
    slot_index = tensor_rank * images + jnp.arange(images)
    image_total = jnp.sum(image_count).astype(jnp.float32)
    image_weight = (
        jnp.where(slot_index < image_count[shard_rank], 1.0, 0.0).astype(jnp.float32) / image_total
    )

    blocks = jnp.concatenate(
        [attn_weight.reshape(LAYERS, 1, own_rows, 4 * attn_width), mlp_weight], axis=1
    ).astype(low)
    widen = lambda values: jnp.pad(
        values, ((0, 0), (0, SMALL_WIDTH - values.shape[1]))
    )
    small = jnp.stack(
        [widen(jnp.concatenate([patch_weight, embed_table], axis=1)), widen(head_weight)]
    ).astype(low)
    weights, small_full, vectors = gather_all(
        blocks.reshape(LAYERS * LAYER_BLOCKS, own_rows, mlp_width),
        small,
        flatten_all([split_vec, hidden_bias]),
    )
    patch_full, table_full = small_full[0, :, :D], small_full[0, :, D : D + EXTRA]
    head_full = small_full[1, :, :CLASSES]
    split_rows = vectors[:, : split_vec.size].reshape(tensor_width, LAYERS, 2, attn_width)
    split_rows = jnp.stack(
        [split_rows[:, :, 0], jnp.zeros_like(split_rows[:, :, 0]), split_rows[:, :, 1]], axis=2
    ).reshape(tensor_width, LAYERS, 1, 3 * attn_width)
    hidden_rows = vectors[:, split_vec.size :].reshape(tensor_width, LAYERS, 1, mlp_width)

    table_rows = table_full.astype(jnp.float32).T
    pixel_rows = patches.reshape(images * (TOK_IMG - 1), PATCH)
    embedded = jnp.dot(pixel_rows, patch_full, preferred_element_type=jnp.float32).reshape(
        images, TOK_IMG - 1, D
    )
    embedded = embedded + table_rows[1:TOK_IMG] + table_rows[TOK_IMG]
    residual = jnp.concatenate(
        [
            jnp.broadcast_to(table_rows[0], (images, 1, D)),
            embedded,
            jnp.zeros((images, PAD_ROWS - TOK_IMG, D), jnp.float32),
        ],
        axis=1,
    ).reshape(images * PAD_ROWS, D)

    saved = []
    for layer_idx in range(LAYERS):
        gains = shared_vec[6 * layer_idx : 6 * layer_idx + 6]
        layer_input = residual
        residual, mid, qkv, mixed, act, slope = forward_layer(
            layer_idx, images, residual, gains, weights,
            split_rows[:, layer_idx], hidden_rows[:, layer_idx],
        )
        saved.append((layer_input, mid, gains, qkv, mixed, act, slope))
    cls_rows = residual.reshape(images, PAD_ROWS, D)[:, 0]
    feature, final_back = jax.vjp(
        layer_norm, cls_rows, shared_vec[6 * LAYERS], shared_vec[6 * LAYERS + 1]
    )
    feature_low = feature.astype(low)
    logits = jnp.dot(feature_low, head_full, preferred_element_type=jnp.float32) + head_bias
    log_norm = jax.nn.logsumexp(logits, axis=-1, keepdims=True)
    onehot = jnp.where(labels[:, None] == jnp.arange(CLASSES)[None, :], 1.0, 0.0).astype(
        jnp.float32
    )
    target = (1.0 - smoothing) * onehot + smoothing / CLASSES
    loss_part = jnp.sum((log_norm[:, 0] - jnp.sum(target * logits, axis=-1)) * image_weight)
    grad_logits = (jnp.exp(logits - log_norm) - target) * image_weight[:, None]
    grad_head_bias = jnp.sum(grad_logits, axis=0)
    logits_low = grad_logits.astype(low)
    grad_head = outer_sum(feature_low, logits_low)
    grad_feature = times_transposed(logits_low, head_full)
    grad_cls, grad_final_gain, grad_final_shift = final_back(grad_feature)
    grad_rows = jnp.concatenate(
        [grad_cls[:, None], jnp.zeros((images, PAD_ROWS - 1, D), jnp.float32)], axis=1
    ).reshape(images * PAD_ROWS, D)
    shared_list = [None] * LAYERS
    split_list = [None] * LAYERS
    hidden_list = [None] * LAYERS
    attn_list = [None] * LAYERS
    mlp_list = [None] * LAYERS
    layer_parts = []
    for layer_idx in reversed(range(LAYERS)):
        layer_input, mid, gains, qkv, mixed, act, slope = saved[layer_idx]
        grad_rows, attn_part, mlp_part, shared_list[layer_idx], split_part, hidden_part = (
            backward_layer(
                layer_idx, images, grad_rows, layer_input, mid, gains, weights,
                qkv, mixed, act, slope,
            )
        )
        split_part = split_part.reshape(tensor_width, 3, attn_width)
        split_list[layer_idx] = jnp.stack([split_part[:, 0], split_part[:, 2]], axis=1)
        hidden_list[layer_idx] = hidden_part.reshape(tensor_width, mlp_width)
        layer_parts.append((attn_part, mlp_part))
    for layer_idx, (attn_sum, mlp_sum) in zip(reversed(range(LAYERS)), sum_layers(layer_parts)):
        attn_list[layer_idx] = attn_sum.reshape(own_rows, 4, attn_width)
        mlp_list[layer_idx] = mlp_sum
    grad_image = grad_rows.reshape(images, PAD_ROWS, D)
    grad_first = jnp.sum(grad_image[:, 0], axis=0)
    grad_position = jnp.sum(grad_image[:, 1:TOK_IMG], axis=0)
    grad_patch_bias = jnp.sum(grad_position, axis=0)
    embed_low = grad_image[:, 1:TOK_IMG].astype(low).reshape(images * (TOK_IMG - 1), D)
    grad_patch = outer_sum(pixel_rows, embed_low)
    grad_table = jnp.concatenate([grad_first[None], grad_position, grad_patch_bias[None]], axis=0).T
    small_sum = sum_small(
        jnp.stack(
            [widen(jnp.concatenate([grad_patch, grad_table], axis=1)), widen(grad_head)]
        ).astype(low)
    )
    patch_grad, table_grad = small_sum[0, :, :D], small_sum[0, :, D : D + EXTRA]
    head_grad = small_sum[1, :, :CLASSES]
    attn_grad = jnp.stack(attn_list)
    mlp_grad = jnp.stack(mlp_list)
    shared_grad = jnp.concatenate(
        shared_list + [jnp.stack([grad_final_gain, grad_final_shift])], axis=0
    )
    attn_sq = attn_grad * attn_grad
    mlp_sq = mlp_grad * mlp_grad
    patch_sq = patch_grad * patch_grad
    table_sq = table_grad * table_grad
    head_sq = head_grad * head_grad

    split_sums, hidden_sums, shared_full, head_bias_full, loss_total = summed_over(
        both,
        [jnp.stack(split_list, 1), jnp.stack(hidden_list, 1), shared_grad, grad_head_bias, loss_part],
    )
    split_total = lax.dynamic_index_in_dim(split_sums, tensor_rank, 0, keepdims=False)
    hidden_total = lax.dynamic_index_in_dim(hidden_sums, tensor_rank, 0, keepdims=False)
    patch_row_new = decay_rate * patch_rows + (1.0 - decay_rate) * (
        jnp.sum(patch_sq, axis=1) / D + tiny_sq
    )
    table_row_new = decay_rate * embed_rows + (1.0 - decay_rate) * (
        jnp.sum(table_sq, axis=1) / EXTRA + tiny_sq
    )
    head_row_new = decay_rate * head_rows + (1.0 - decay_rate) * (
        jnp.sum(head_sq, axis=1) / CLASSES + tiny_sq
    )
    own_share = 1.0 / tensor_width
    (
        (
            patch_col_full, table_col_full, head_col_full, whole_row_sum,
            attn_old_sum, mlp_old_sum, attn_total, mlp_total, weight_sq_parts,
        ),
        (attn_row_full, mlp_row_full),
        (attn_col_full, mlp_col_full),
    ) = sums_over(
        [
            (
                "both",
                [
                    jnp.sum(patch_sq, axis=0),
                    jnp.sum(table_sq, axis=0),
                    jnp.sum(head_sq, axis=0),
                    jnp.stack(
                        [jnp.sum(patch_row_new), jnp.sum(table_row_new), jnp.sum(head_row_new)]
                    ),
                    jnp.sum(attn_rows, axis=-1) * own_share,
                    jnp.sum(mlp_rows, axis=-1) * own_share,
                    jnp.sum(attn_sq, axis=(1, 3)),
                    jnp.sum(mlp_sq, axis=(2, 3)),
                    flatten_all(
                        [
                            jnp.sum(attn_weight * attn_weight, axis=(1, 3)),
                            jnp.sum(mlp_weight * mlp_weight, axis=(2, 3)),
                            jnp.sum(patch_weight * patch_weight),
                            jnp.sum(embed_table * embed_table),
                            jnp.sum(head_weight * head_weight),
                        ]
                    ),
                ],
            ),
            ("tensor", [jnp.sum(attn_sq, axis=3).transpose(0, 2, 1), jnp.sum(mlp_sq, axis=3)]),
            ("dp", [jnp.sum(attn_sq, axis=1), jnp.sum(mlp_sq, axis=2)]),
        ],
        4,
    )
    attn_row_new = decay_rate * attn_rows + (1.0 - decay_rate) * (attn_row_full / D + tiny_sq)
    mlp_row_new = decay_rate * mlp_rows + (1.0 - decay_rate) * (mlp_row_full / FF + tiny_sq)
    weight_sq = split_all(weight_sq_parts, [(LAYERS, 4), (LAYERS, 2), (), (), ()])
    attn_row_mean = (
        decay_rate * attn_old_sum + (1.0 - decay_rate) * (attn_total / D + D * tiny_sq)
    ) / D
    mlp_row_mean = (
        decay_rate * mlp_old_sum + (1.0 - decay_rate) * (mlp_total / FF + D * tiny_sq)
    ) / D
    whole_row_mean = whole_row_sum / jnp.array([PATCH, D, D], jnp.float32)
    attn_col_new = decay_rate * attn_cols + (1.0 - decay_rate) * (attn_col_full / D + tiny_sq)
    mlp_col_new = decay_rate * mlp_cols + (1.0 - decay_rate) * (mlp_col_full / D + tiny_sq)
    patch_col_new = decay_rate * patch_cols + (1.0 - decay_rate) * (
        patch_col_full / PATCH + tiny_sq
    )
    table_col_new = decay_rate * embed_cols + (1.0 - decay_rate) * (table_col_full / D + tiny_sq)
    head_col_new = decay_rate * head_cols + (1.0 - decay_rate) * (head_col_full / D + tiny_sq)
    attn_update = attn_grad * lax.rsqrt(
        attn_row_new.transpose(0, 2, 1)[:, :, :, None]
        * attn_col_new[:, None]
        / attn_row_mean[:, None, :, None]
    )
    mlp_update = mlp_grad * lax.rsqrt(
        mlp_row_new[:, :, :, None] * mlp_col_new[:, :, None, :] / mlp_row_mean[:, :, None, None]
    )
    patch_update = patch_grad * lax.rsqrt(
        patch_row_new[:, None] * patch_col_new[None, :] / whole_row_mean[0]
    )
    table_update = table_grad * lax.rsqrt(
        table_row_new[:, None] * table_col_new[None, :] / whole_row_mean[1]
    )
    head_update = head_grad * lax.rsqrt(
        head_row_new[:, None] * head_col_new[None, :] / whole_row_mean[2]
    )
    split_sq_new = decay_rate * split_sq + (1.0 - decay_rate) * (
        split_total * split_total + tiny_sq
    )
    split_update = split_total * lax.rsqrt(split_sq_new)
    hidden_sq_new = decay_rate * hidden_sq + (1.0 - decay_rate) * (
        hidden_total * hidden_total + tiny_sq
    )
    hidden_update = hidden_total * lax.rsqrt(hidden_sq_new)
    shared_sq_new = decay_rate * shared_sq + (1.0 - decay_rate) * (
        shared_full * shared_full + tiny_sq
    )
    shared_update = shared_full * lax.rsqrt(shared_sq_new)
    head_bias_sq_new = decay_rate * head_bias_sq + (1.0 - decay_rate) * (
        head_bias_full * head_bias_full + tiny_sq
    )
    head_bias_update = head_bias_full * lax.rsqrt(head_bias_sq_new)
    dp_share = 1.0 / dp_width
    ((attn_u2, mlp_u2, patch_u2, table_u2, head_u2, split_u2, hidden_u2, split_w2, hidden_w2),) = (
        sums_over(
            [("both", [
                jnp.sum(attn_update * attn_update, axis=(1, 3)),
                jnp.sum(mlp_update * mlp_update, axis=(2, 3)),
                jnp.sum(patch_update * patch_update),
                jnp.sum(table_update * table_update),
                jnp.sum(head_update * head_update),
                jnp.sum(split_update * split_update, axis=-1) * dp_share,
                jnp.sum(hidden_update * hidden_update, axis=-1) * dp_share,
                jnp.sum(split_vec * split_vec, axis=-1) * dp_share,
                jnp.sum(hidden_bias * hidden_bias, axis=-1) * dp_share,
            ])],
            5,
        )
    )
    vector_sq = [split_w2, hidden_w2]
    attn_new = finish_step(
        attn_weight, attn_update, attn_u2[:, None, :, None], weight_sq[0][:, None, :, None], D * D
    )
    mlp_new = finish_step(
        mlp_weight, mlp_update, mlp_u2[:, :, None, None], weight_sq[1][:, :, None, None], D * FF
    )
    patch_new = finish_step(patch_weight, patch_update, patch_u2, weight_sq[2], PATCH * D)
    embed_new = finish_step(embed_table, table_update, table_u2, weight_sq[3], D * EXTRA)
    head_new = finish_step(head_weight, head_update, head_u2, weight_sq[4], D * CLASSES)
    split_new = finish_step(
        split_vec, split_update, split_u2[:, :, None], vector_sq[0][:, :, None], D
    )
    hidden_new = finish_step(
        hidden_bias, hidden_update, hidden_u2[:, None], vector_sq[1][:, None], FF
    )
    shared_new = finish_step(
        shared_vec,
        shared_update,
        jnp.sum(shared_update * shared_update, axis=-1, keepdims=True),
        jnp.sum(shared_vec * shared_vec, axis=-1, keepdims=True),
        D,
    )
    head_bias_new = finish_step(
        head_bias,
        head_bias_update,
        jnp.sum(head_bias_update * head_bias_update),
        jnp.sum(head_bias * head_bias),
        CLASSES,
    )
    return (
        loss_total,
        attn_new,
        attn_row_new,
        attn_col_new,
        mlp_new,
        mlp_row_new,
        mlp_col_new,
        patch_new,
        patch_row_new,
        patch_col_new,
        embed_new,
        table_row_new,
        table_col_new,
        head_new,
        head_row_new,
        head_col_new,
        split_new,
        split_sq_new,
        hidden_new,
        hidden_sq_new,
        shared_new,
        shared_sq_new,
        head_bias_new,
        head_bias_sq_new,
    )


def solution(mesh):
    in_specs = (
        P(("dp", "tensor"), None, None),
        P(("dp", "tensor")),
        P(),
        P(None, "dp", None, "tensor"),
        P(None, None, "dp"),
        P(None, None, "tensor"),
        P(None, None, "dp", "tensor"),
        P(None, None, "dp"),
        P(None, None, "tensor"),
        P(("dp", "tensor"), None),
        P(("dp", "tensor")),
        P(),
        P(("dp", "tensor"), None),
        P(("dp", "tensor")),
        P(),
        P(("dp", "tensor"), None),
        P(("dp", "tensor")),
        P(),
        P(None, None, "tensor"),
        P(None, None, "tensor"),
        P(None, "tensor"),
        P(None, "tensor"),
        P(),
        P(),
        P(),
        P(),
    )
    out_specs = (
        P(),
        P(None, "dp", None, "tensor"),
        P(None, None, "dp"),
        P(None, None, "tensor"),
        P(None, None, "dp", "tensor"),
        P(None, None, "dp"),
        P(None, None, "tensor"),
        P(("dp", "tensor"), None),
        P(("dp", "tensor")),
        P(),
        P(("dp", "tensor"), None),
        P(("dp", "tensor")),
        P(),
        P(("dp", "tensor"), None),
        P(("dp", "tensor")),
        P(),
        P(None, None, "tensor"),
        P(None, None, "tensor"),
        P(None, "tensor"),
        P(None, "tensor"),
        P(),
        P(),
        P(),
        P(),
    )
    return jax.shard_map(shards, mesh=mesh, in_specs=in_specs, out_specs=out_specs, check_vma=False)
```
